32 devices in a mesh: rot: 2 (over y), py: 4 (over x, core), pz: 4 (over z).
Axes of the slice: x: 2, y: 2, z: 4, core: 2. Of those that a mesh axis runs over, the one named last changes fastest.
Arguments:
- receptor_grids: float32 [2, 128, 128, 128], P('rot', None, 'py', 'pz'), may hold values from -0.09375 to 0.09375
- ligand_cells: int32 [8, 2048], P('rot'), may hold values from 0 to 2097151
- atom_shape: float32 [2048], replicated, may hold values from 0.5 to 2
- atom_charges: float32 [2048], replicated, may hold values from -3 to 3
Outputs:
- correlation: float32 [8, 128, 128, 128], P('rot', 'py', 'pz')
- best_score: float32 [8], P('rot')
The draws below stay inside these ranges and needn't reach their ends.
Inputs may be any that keep to these rules, and one draw needn't show every extreme that they name: Atom a of rotation r lies in cell (x, y, z) with ligand_cells[r, a] = x 128^2 + y * 128 + z; several atoms may share a cell.
All inputs are finite; a program needn't handle non-finite values.
Results may differ from the reference program's by a relative error of at most 0.000086.
Values sent between devices are 32-bit elements; how exact they have to be, the bound alone decides.
No kernel may reach another device: no remote copies, remote signals or barrier semaphores. Data moves between devices by JAX's collectives and lax.ppermute only.
A program may use at most 192 MiB of HBM per device.

```python
import math
import jax
import jax.numpy as jnp
from jax import lax

N = 128
ATOMS = 2048
ROTATIONS = 8


def touch_ends(drawn, own_key, least, largest):
    place = [jax.random.randint(jax.random.fold_in(own_key, axis), (), 0, length) for axis, length in enumerate(drawn.shape)]
    widest = drawn.shape.index(max(drawn.shape))
    neighbour = place[:widest] + [(place[widest] + 1) % drawn.shape[widest]] + place[widest + 1:]
    return drawn.at[tuple(place)].set(least).at[tuple(neighbour)].set(largest)


def shard_levels(stream_key, dims, split, low, largest):
    loudness, own = 1.0, jax.random.fold_in(stream_key, 6)
    for axis_at, shards_of in split:
        heights = jnp.exp(jax.random.uniform(jax.random.fold_in(own, axis_at), (shards_of,), jnp.float32, low / len(split), largest / len(split)))
        loudness = loudness * jnp.repeat(heights, dims[axis_at] // shards_of).reshape([-1 if axis == axis_at else 1 for axis in range(len(dims))])
    return loudness


def scatter_about(own_key, extent, width, reach, pieces=(), kind=jnp.bfloat16):
    gain = shard_levels(own_key, extent, pieces, -0.22, 0.18) if pieces else 1.0
    drawn = jax.random.normal(own_key, extent, jnp.float32) * width * gain
    return jnp.minimum(jnp.maximum(drawn, -reach), reach).astype(kind)


def setup_inputs(seed: int = 0) -> dict:
    key_of = jax.random.split(jax.random.key(seed), 5)
    receptor_grids = scatter_about(key_of[0], (2, N, N, N), (2 * ATOMS) ** -0.5, 0.09375, ((0, 2), (2, 4), (3, 4)), jnp.float32)
    ligand_cells = touch_ends(jax.random.randint(key_of[1], (ROTATIONS, ATOMS), 0, N ** 3), jax.random.fold_in(key_of[1], 1), 0, (N ** 3) - 1).astype(jnp.int32)
    atom_shape = jnp.clip(jnp.exp(jax.random.uniform(key_of[2], (ATOMS,), jnp.float32, math.log(0.5), math.log(2.0))), 0.5, 2.0)
    atom_charges = scatter_about(key_of[3], (ATOMS,), 0.5, 3.0, (), jnp.float32)
    return dict(receptor_grids=receptor_grids, ligand_cells=ligand_cells, atom_shape=atom_shape, atom_charges=atom_charges)


def reference(receptor_grids, ligand_cells, atom_shape, atom_charges):
    receptor_spectrum = jnp.fft.fftn(receptor_grids, axes=(1, 2, 3))
    weights = jnp.stack((atom_shape, atom_charges), 0)

    def single_rotation(atom_cells):
        ligand_grids = jnp.zeros((2, N * N * N), jnp.float32).at[:, atom_cells].add(weights)
        ligand_spectrum = jnp.fft.fftn(ligand_grids.reshape(2, N, N, N), axes=(1, 2, 3))
        product = jnp.sum(receptor_spectrum * jnp.conj(ligand_spectrum), axis=0)
        grid_map = jnp.real(jnp.fft.ifftn(product)).astype(jnp.float32)
        return jnp.transpose(grid_map, (1, 2, 0))

    correlation = lax.map(single_rotation, ligand_cells)
    best_score = jnp.max(correlation, axis=(1, 2, 3))
    return correlation, best_score
```

```python
import functools
import math

import jax
import jax.numpy as jnp
import numpy as np
from jax import lax
from jax.experimental import pallas as pl
from jax.experimental.pallas import tpu as pltpu
from jax.sharding import PartitionSpec as P

exact_mode = lax.Precision.HIGHEST
AXES = ("rot", "py", "pz")
LANES = 128
SUBLANES = 8


def split_constant(matrix):
    head = np.asarray(matrix, np.float64).astype(jnp.bfloat16)
    rest = (np.asarray(matrix, np.float64) - head.astype(np.float64)).astype(jnp.bfloat16)
    return head, rest


def plus_matrix(n):
    turns = np.outer(np.arange(n), np.arange(n)) % n
    cosine, sine = np.cos(turns * (2 * np.pi / n)), np.sin(turns * (2 * np.pi / n))
    return np.block([[cosine, sine], [-sine, cosine]])


def component_phases(n):
    places = np.arange(n)
    phases = np.zeros((n, n), np.int64)
    for slot in range(n // 2):
        phases[2 * slot] = slot * places % n
        phases[2 * slot + 1] = (n // 2) * places % n if slot == 0 else (slot * places - n // 4) % n
    return phases


def forward_x_matrix(n):
    return np.cos(component_phases(n) * (2 * np.pi / n))


def inverse_x_matrix(n):
    matrix = np.cos(component_phases(n) * (2 * np.pi / n))
    scale = np.full((n, 1), 2.0)
    scale[3::2] = -2.0
    scale[:2] = 1.0
    return matrix * scale / float(n) ** 3


def split(value):
    head = value.astype(jnp.bfloat16)
    rest = (value - head.astype(jnp.float32)).astype(jnp.bfloat16)
    return head, rest


def dot(a, b):
    return jnp.dot(a, b, preferred_element_type=jnp.float32)


def times_constant(value, head_ref, rest_ref):
    head, rest = split(value)
    return dot(head, head_ref[...]) + (dot(head, rest_ref[...]) + dot(rest, head_ref[...]))


def constant_times(head_ref, rest_ref, value):
    head, rest = split(value)
    return dot(head_ref[...], head) + (dot(rest_ref[...], head) + dot(head_ref[...], rest))


def swap_groups(pieces, width):
    return [
        jnp.concatenate([piece[..., q * width : (q + 1) * width] for piece in pieces], axis=-1)
        for q in range(len(pieces))
    ]


def forward_x_kernel(grid_ref, head_ref, rest_ref, out_ref, rows_ref):
    n, y_block, z_block = grid_ref.shape[1:]
    groups = LANES // z_block
    high = y_block // groups
    rows_ref[...] = jnp.concatenate(
        [grid_ref[0, :, g * high : (g + 1) * high, :] for g in range(groups)], axis=-1
    ).reshape(n * high, LANES)
    for row in range(high):
        values = rows_ref[pl.ds(row, n, stride=high), :]
        out_ref[pl.ds(row, n, stride=high), :] = constant_times(head_ref, rest_ref, values)


def spectrum(planes, n, zh, zr, yh, yr):
    count = len(planes)
    rows = jnp.concatenate([jnp.concatenate(pair, axis=1) for pair in planes], axis=0)
    rows = times_constant(rows, zh, zr)
    columns = jnp.concatenate(
        [
            jnp.concatenate([rows[i * n : (i + 1) * n, :n], rows[i * n : (i + 1) * n, n:]], axis=0)
            for i in range(count)
        ],
        axis=1,
    )
    return constant_times(yh, yr, columns)


def ligand_kernel(special_ref, values_ref, cell_ref, zh, zr, yh, yr, out_ref):
    n = zh.shape[0] // 2
    comps, atoms = values_ref.shape[-2:]
    half = n // 2
    special = special_ref[0, 0] > 0
    grids = []
    for rotation in range(2):
        cell = cell_ref[0, rotation : rotation + 1, :]
        y_low = (cell // n) % half
        place = cell % n + n * ((cell // (n * half)) % 2)
        head = values_ref[0, rotation].astype(jnp.bfloat16).astype(jnp.float32)
        rest = (values_ref[0, rotation] - head).astype(jnp.bfloat16).astype(jnp.float32)
        hit = lax.broadcasted_iota(jnp.int32, (half, atoms), 0) == y_low
        stacked = jnp.concatenate(
            [
                jnp.where(hit, part[c : c + 1, :], 0.0).astype(jnp.bfloat16)
                for part in (head, rest)
                for c in range(comps)
            ],
            axis=0,
        )
        one_hot = (
            lax.broadcasted_iota(jnp.int32, (2 * n, atoms), 0) == place
        ).astype(jnp.float32).astype(jnp.bfloat16)
        total = lax.dot_general(
            stacked, one_hot, (((1,), (1,)), ((), ())), preferred_element_type=jnp.float32
        )
        total = total[: comps * half] + total[comps * half :]
        grids.append(
            [
                jnp.concatenate(
                    [total[c * half : (c + 1) * half, :n], total[c * half : (c + 1) * half, n:]], axis=0
                )
                for c in range(comps)
            ]
        )
    planes = [[], []]
    for c in range(0, comps, 2):
        first, second = (grids[0][c], grids[0][c + 1]), (grids[1][c], grids[1][c + 1])
        if c < 4:
            first, second = (
                (first[0], jnp.where(special, second[0], first[1])),
                (jnp.where(special, first[1], second[0]), second[1]),
            )
        planes[0].append(first)
        planes[1].append(second)
    out_ref[0] = spectrum(planes[0] + planes[1], n, zh, zr, yh, yr)


def receptor_kernel(special_ref, blocks_ref, zh, zr, yh, yr, out_ref, *, channels, y_parts, z_parts):
    n = zh.shape[0] // 2
    width = n // z_parts
    comps = blocks_ref.shape[1] // SUBLANES
    special = special_ref[0, 0] > 0
    planes = []
    for channel in range(channels):
        parts = []
        for c in range(comps):
            rows = []
            for y_part in range(y_parts):
                first = (channel * y_parts + y_part) * z_parts
                pieces = [blocks_ref[first + i, c * SUBLANES : (c + 1) * SUBLANES, :] for i in range(z_parts)]
                rows += swap_groups(pieces, width)
            parts.append(jnp.concatenate(rows, axis=0))
        zero = jnp.zeros_like(parts[0])
        lone = jnp.where(special, zero, parts[1])
        planes.append((parts[0], lone))
        planes.append((jnp.where(special, parts[1], parts[0]), lone))
        for c in range(2, comps, 2):
            planes.append((parts[c], parts[c + 1]))
    out_ref[...] = spectrum(planes, n, zh, zr, yh, yr)


def product_kernel(special_ref, receptor_ref, ligand_ref, zh, zr, yh, yr, out_ref, *, channels, y_parts, z_parts):
    n = zh.shape[0] // 2
    width = n // z_parts
    groups = LANES // width
    slots = ligand_ref.shape[2] // (2 * channels * n)
    special = special_ref[0, 0] > 0

    def receptor(channel, slot, rotation):
        at = channel * (slots + 1) + (rotation if slot == 0 else slot + 1)
        return receptor_ref[:n, at * n : (at + 1) * n], receptor_ref[n:, at * n : (at + 1) * n]

    def ligand(channel, slot, rotation):
        at = (rotation * slots + slot) * channels + channel
        return ligand_ref[0, :n, at * n : (at + 1) * n], ligand_ref[0, n:, at * n : (at + 1) * n]

    columns = []
    for rotation in range(2):
        for slot in range(slots):
            real, imag = 0.0, 0.0
            for channel in range(channels):
                fr, fi = receptor(channel, slot, rotation)
                hr, hi = ligand(channel, slot, rotation)
                real = real + (fr * hr + fi * hi)
                imag = imag + (fr * hi - fi * hr)
            columns.append(jnp.concatenate([real, imag], axis=0))
    columns = constant_times(yh, yr, jnp.concatenate(columns, axis=1))
    rows = jnp.concatenate(
        [
            jnp.concatenate([columns[:n, i * n : (i + 1) * n], columns[n:, i * n : (i + 1) * n]], axis=1)
            for i in range(2 * slots)
        ],
        axis=0,
    )
    rows = times_constant(rows, zh, zr)
    maps = [
        [
            [rows[(rotation * slots + slot) * n : (rotation * slots + slot + 1) * n, p * n : (p + 1) * n] for p in range(2)]
            for slot in range(slots)
        ]
        for rotation in range(2)
    ]
    lone, other = maps[0][0][1], maps[1][0][0]
    maps[0][0][1] = jnp.where(special, other, lone)
    maps[1][0][0] = jnp.where(special, lone, other)
    for rotation in range(2):
        for slot in range(slots):
            for p in range(2):
                plane = maps[rotation][slot][p]
                row = (slot * 2 + p) * SUBLANES
                for y_part in range(y_parts):
                    pieces = [
                        plane[(y_part * groups + g) * SUBLANES : (y_part * groups + g + 1) * SUBLANES, :]
                        for g in range(groups)
                    ]
                    for z_part, block in enumerate(swap_groups(pieces, width)):
                        out_ref[(rotation * y_parts + y_part) * z_parts + z_part, row : row + SUBLANES, :] = block


def inverse_x_kernel(blocks_ref, head_ref, rest_ref, out_ref, best_ref):
    n = head_ref.shape[0]
    y_block, z_block = out_ref.shape[1:3]
    groups = LANES // z_block
    best = None
    for row in range(SUBLANES):
        values = blocks_ref[0, pl.ds(row, n, stride=SUBLANES), :]
        result = times_constant(values.T, head_ref, rest_ref)
        for g in range(groups):
            out_ref[0, g * SUBLANES + row] = result[g * z_block : (g + 1) * z_block, :]
        best = result if best is None else jnp.maximum(best, result)
    best_ref[0] = jnp.broadcast_to(jnp.max(best, axis=(0, 1), keepdims=True), (SUBLANES, LANES))


def whole():
    return pl.BlockSpec(memory_space=pltpu.VMEM)


def scalar():
    return pl.BlockSpec(memory_space=pltpu.SMEM)


def on_device(receptor_grids, ligand_cells, atom_shape, atom_charges, *, sizes):
    n = receptor_grids.shape[1]
    rots, y_parts, z_parts = (sizes[a] for a in AXES)
    devices = rots * y_parts * z_parts
    slots = n // 2 // devices
    comps = 2 * slots
    y_block, z_block = receptor_grids.shape[2:]
    rotations, atoms = ligand_cells.shape
    channels = 2
    planes = [jnp.asarray(m) for m in split_constant(plus_matrix(n))]
    planes += [m.T for m in (np.asarray(p) for p in split_constant(plus_matrix(n)))]
    planes = [jnp.asarray(m) for m in planes]
    f32 = jnp.float32

    other = lax.ppermute(ligand_cells, "rot", [(i, i ^ 1) for i in range(rots)])

    components = pl.pallas_call(
        forward_x_kernel,
        out_shape=jax.ShapeDtypeStruct((n * SUBLANES, LANES), f32),
        in_specs=[whole()] * 3,
        out_specs=whole(),
        scratch_shapes=[pltpu.VMEM((n * SUBLANES, LANES), f32)],
        name="forward_x",
    )(receptor_grids, *(jnp.asarray(m) for m in split_constant(forward_x_matrix(n))))
    blocks = lax.all_to_all(components.reshape(devices, comps * SUBLANES, LANES), AXES, 0, 0, tiled=True)

    mine = lax.axis_index("rot") == 0
    cells = jnp.stack(
        [jnp.where(mine, ligand_cells, other), jnp.where(mine, other, ligand_cells)], axis=1
    )
    device = lax.axis_index(AXES)
    coord_x = cells // (n * n)
    slot = device * slots + jnp.arange(slots, dtype=jnp.int32)
    turns = slot[:, None] * coord_x[:, :, None, None, :]
    quarter = jnp.where(
        slot[:, None] == 0, (n // 2) * coord_x[:, :, None, None, :], turns - n // 4
    )
    phase = jnp.concatenate([turns[..., None, :], quarter[..., None, :]], axis=-2) % n
    wave = jnp.cos(phase.astype(f32) * (2.0 * math.pi / n))
    weights = jnp.stack([atom_shape, atom_charges], 0)[:, None, :]
    wave = jnp.swapaxes(wave, 2, 3) if wave.shape[2] == 1 else wave
    wave = wave.reshape(rotations, rots, slots, 1, 2, atoms)
    values = (wave * weights).reshape(rotations, rots, slots * channels * 2, atoms)
    special = (device == 0).astype(jnp.int32).reshape(1, 1)

    width = 2 * slots * channels * n
    ligand = pl.pallas_call(
        ligand_kernel,
        grid=(rotations,),
        out_shape=jax.ShapeDtypeStruct((rotations, 2 * n, width), f32),
        in_specs=[
            scalar(),
            pl.BlockSpec((1, rots, slots * channels * 2, atoms), lambda i: (i, 0, 0, 0)),
            pl.BlockSpec((1, rots, atoms), lambda i: (i, 0, 0)),
        ]
        + [whole()] * 4,
        out_specs=pl.BlockSpec((1, 2 * n, width), lambda i: (i, 0, 0)),
        name="ligand",
    )(special, values, cells, *planes)

    receptor = pl.pallas_call(
        functools.partial(receptor_kernel, channels=channels, y_parts=y_parts, z_parts=z_parts),
        out_shape=jax.ShapeDtypeStruct((2 * n, channels * (slots + 1) * n), f32),
        in_specs=[scalar()] + [whole()] * 5,
        out_specs=whole(),
        name="receptor",
    )(special, blocks, *planes)

    rows = comps * SUBLANES
    sent = pl.pallas_call(
        functools.partial(product_kernel, channels=channels, y_parts=y_parts, z_parts=z_parts),
        grid=(rotations,),
        out_shape=jax.ShapeDtypeStruct((devices, rotations * rows, LANES), f32),
        in_specs=[scalar(), whole(), pl.BlockSpec((1, 2 * n, width), lambda i: (i, 0, 0))] + [whole()] * 4,
        out_specs=pl.BlockSpec((devices, rows, LANES), lambda i: (0, i, 0)),
        name="product",
    )(special, receptor, ligand, *planes)
    got = lax.all_to_all(sent, AXES, 0, 0, tiled=True)
    got = jnp.swapaxes(got.reshape(devices, rotations, rows, LANES), 0, 1).reshape(rotations, devices * rows, LANES)

    correlation, best = pl.pallas_call(
        inverse_x_kernel,
        grid=(rotations,),
        out_shape=[
            jax.ShapeDtypeStruct((rotations, y_block, z_block, n), f32),
            jax.ShapeDtypeStruct((rotations, SUBLANES, LANES), f32),
        ],
        in_specs=[pl.BlockSpec((1, devices * rows, LANES), lambda i: (i, 0, 0))] + [whole()] * 2,
        out_specs=[
            pl.BlockSpec((1, y_block, z_block, n), lambda i: (i, 0, 0, 0)),
            pl.BlockSpec((1, SUBLANES, LANES), lambda i: (i, 0, 0)),
        ],
        name="inverse_x",
    )(got, *(jnp.asarray(m) for m in split_constant(inverse_x_matrix(n))))
    best = best[:, 0, :]
    for axis in ("py", "pz"):
        step = 1
        while step < sizes[axis]:
            best = jnp.maximum(best, lax.ppermute(best, axis, [(i, i ^ step) for i in range(sizes[axis])]))
            step *= 2
    return correlation, best[:, 0]


def twiddle(length, inverse):
    counter = jnp.arange(length, dtype=jnp.int32)
    phases = counter[:, None] * counter[None, :] % length
    angles = phases.astype(jnp.float32) * (2.0 * math.pi / length)
    factor = 1.0 if inverse else -1.0
    return (jnp.cos(angles), factor * jnp.sin(angles))


def transform(real_part, imag_part, pattern, inverse, n):
    cosine, sine_table = twiddle(n, inverse)
    if imag_part is None:
        return (
            jnp.einsum(pattern, real_part, cosine, precision=exact_mode),
            jnp.einsum(pattern, real_part, sine_table, precision=exact_mode),
        )
    new_real = jnp.einsum(pattern, real_part, cosine, precision=exact_mode) - jnp.einsum(
        pattern, imag_part, sine_table, precision=exact_mode
    )
    new_imag = jnp.einsum(pattern, real_part, sine_table, precision=exact_mode) + jnp.einsum(
        pattern, imag_part, cosine, precision=exact_mode
    )
    return (new_real, new_imag)


def exchange(pair, axis, split_axis, concat_axis):
    return tuple(lax.all_to_all(p, axis, split_axis=split_axis, concat_axis=concat_axis, tiled=True) for p in pair)


def on_any_device(receptor_grids, ligand_cells, atom_shape, atom_charges, *, sizes):
    n = receptor_grids.shape[1]
    planes = lax.all_gather(receptor_grids, "rot", axis=0, tiled=True)
    pair = transform(planes, None, "cxyz,xk->ckyz", False, n)
    pair = transform(*exchange(pair, "pz", 1, 3), "cxyz,zk->cxyk", False, n)
    receptor_real, receptor_imag = transform(*exchange(pair, "py", 3, 2), "cxyz,yk->cxkz", False, n)
    x_block = n // sizes["pz"]
    z_block = n // sizes["py"]
    kx_values = lax.axis_index("pz") * x_block + jnp.arange(x_block, dtype=jnp.int32)
    kz_values = lax.axis_index("py") * z_block + jnp.arange(z_block, dtype=jnp.int32)
    ky_values = jnp.arange(n, dtype=jnp.int32)
    weights = jnp.stack((atom_shape, atom_charges), 1)
    step_angle = 2.0 * math.pi / n

    def rotation_product(atom_cells):
        coord_x = atom_cells // (n * n)
        coord_y = atom_cells // n % n
        coord_z = atom_cells % n
        angle_y = (coord_y[:, None] * ky_values[None, :] % n).astype(jnp.float32) * step_angle
        cos_y = jnp.cos(angle_y)
        sin_y = jnp.sin(angle_y)
        phase_xz = (
            coord_x[:, None, None] * kx_values[None, :, None]
            + coord_z[:, None, None] * kz_values[None, None, :]
        ) % n
        angle_xz = phase_xz.astype(jnp.float32) * step_angle
        cos_xz = (weights[:, :, None, None] * jnp.cos(angle_xz)[:, None]).reshape(atom_cells.shape[0], -1)
        sin_xz = (weights[:, :, None, None] * jnp.sin(angle_xz)[:, None]).reshape(atom_cells.shape[0], -1)
        meet = functools.partial(jnp.einsum, "ay,ab->yb", precision=exact_mode)
        conj_real = (meet(cos_y, cos_xz) - meet(sin_y, sin_xz)).reshape(n, 2, x_block, z_block)
        conj_imag = (meet(cos_y, sin_xz) + meet(sin_y, cos_xz)).reshape(n, 2, x_block, z_block)
        join = functools.partial(jnp.einsum, "ycxz,cxyz->xyz", precision=exact_mode)
        product_real = join(conj_real, receptor_real) - join(conj_imag, receptor_imag)
        product_imag = join(conj_imag, receptor_real) + join(conj_real, receptor_imag)
        return (product_real, product_imag)

    product_real, product_imag = lax.map(rotation_product, ligand_cells)
    rotations = ligand_cells.shape[0]
    pair_real = product_real.reshape((rotations // 2, 2) + product_real.shape[1:])
    pair_imag = product_imag.reshape((rotations // 2, 2) + product_imag.shape[1:])
    pair = (pair_real[:, 0] - pair_imag[:, 1], pair_imag[:, 0] + pair_real[:, 1])
    pair = transform(*pair, "bxyz,yk->bxkz", True, n)
    pair = transform(*exchange(pair, "py", 2, 3), "bxyz,zk->bxyk", True, n)
    even_maps, odd_maps = transform(*exchange(pair, "pz", 3, 1), "bxyz,xk->byzk", True, n)
    stacked = jnp.stack((even_maps, odd_maps), 1)
    correlation = stacked.reshape((rotations,) + even_maps.shape[1:]) * (1.0 / (n * n * n))
    best_score = lax.pmax(jnp.max(correlation, axis=(1, 2, 3)), ("py", "pz"))
    return (correlation, best_score)


def solution(mesh):
    sizes = dict(mesh.shape)

    def run(receptor_grids, ligand_cells, atom_shape, atom_charges):
        n = receptor_grids.shape[1]
        devices = math.prod(sizes[a] for a in AXES)
        fits = (
            sizes["rot"] == 2
            and n == LANES
            and (n // 2) % devices == 0
            and (n // sizes["py"]) * (n // sizes["pz"]) == SUBLANES * LANES
            and all(sizes[a] & (sizes[a] - 1) == 0 for a in AXES)
        )
        body = functools.partial(on_device if fits else on_any_device, sizes=sizes)
        placed = (P("rot", None, "py", "pz"), P("rot", None), P(), P())
        return jax.shard_map(
            body,
            mesh=mesh,
            in_specs=placed,
            out_specs=(P("rot", "py", "pz", None), P("rot")),
            check_vma=False,
        )(receptor_grids, ligand_cells, atom_shape, atom_charges)

    return run
```

```python
import functools
import math

import jax
import jax.numpy as jnp
import numpy as np
from jax import lax
from jax.experimental import pallas as pl
from jax.experimental.pallas import tpu as pltpu
from jax.sharding import PartitionSpec as P

exact_mode = lax.Precision.HIGHEST
AXES = ("rot", "py", "pz")
LANES = 128
SUBLANES = 8


def split_constant(matrix):
    head = np.asarray(matrix, np.float64).astype(jnp.bfloat16)
    rest = (np.asarray(matrix, np.float64) - head.astype(np.float64)).astype(jnp.bfloat16)
    return head, rest


def plus_matrix(n):
    turns = np.outer(np.arange(n), np.arange(n)) % n
    cosine, sine = np.cos(turns * (2 * np.pi / n)), np.sin(turns * (2 * np.pi / n))
    return np.block([[cosine, sine], [-sine, cosine]])


def component_phases(n):
    places = np.arange(n)
    phases = np.zeros((n, n), np.int64)
    for slot in range(n // 2):
        phases[2 * slot] = slot * places % n
        phases[2 * slot + 1] = (n // 2) * places % n if slot == 0 else (slot * places - n // 4) % n
    return phases


def forward_x_matrix(n):
    return np.cos(component_phases(n) * (2 * np.pi / n))


def inverse_x_matrix(n):
    matrix = np.cos(component_phases(n) * (2 * np.pi / n))
    scale = np.full((n, 1), 2.0)
    scale[3::2] = -2.0
    scale[:2] = 1.0
    return matrix * scale / float(n) ** 3


def split(value):
    head = value.astype(jnp.bfloat16)
    rest = (value - head.astype(jnp.float32)).astype(jnp.bfloat16)
    return head, rest


def dot(a, b):
    return jnp.dot(a, b, preferred_element_type=jnp.float32)


def dot_rows(a, b):
    return lax.dot_general(a, b, (((1,), (1,)), ((), ())), preferred_element_type=jnp.float32)


def times_constant(value, head_ref, rest_ref):
    head, rest = split(value)
    return dot(head, head_ref[...]) + (dot(head, rest_ref[...]) + dot(rest, head_ref[...]))


def constant_times(head_ref, rest_ref, values):
    results = []
    for i in range(0, len(values), 2):
        pair = values[i : i + 2]
        head, rest = split(jnp.concatenate(pair, axis=1))
        result = dot(head_ref[...], head) + (dot(rest_ref[...], head) + dot(head_ref[...], rest))
        width = pair[0].shape[1]
        results += [result[:, j * width : (j + 1) * width] for j in range(len(pair))]
    return results


def swap_groups(pieces, width):
    pieces = list(pieces)
    lane = lax.broadcasted_iota(jnp.int32, pieces[0].shape, 1)
    bit = len(pieces) // 2
    while bit:
        low = lane // (bit * width) % 2 == 0
        for i in range(len(pieces)):
            if i & bit == 0:
                first, second = pieces[i], pieces[i | bit]
                pieces[i] = jnp.where(low, first, pltpu.roll(second, bit * width, 1))
                pieces[i | bit] = jnp.where(low, pltpu.roll(first, LANES - bit * width, 1), second)
        bit //= 2
    return pieces


def forward_x_kernel(grid_ref, head_ref, rest_ref, out_ref):
    y_block, z_block, n = grid_ref.shape[1:]
    groups = LANES // z_block
    high = y_block // groups
    for row in range(high):
        values = jnp.concatenate([grid_ref[0, g * high + row] for g in range(groups)], axis=0)
        head, rest = split(values)
        out_ref[pl.ds(row, n, stride=high), :] = dot_rows(head_ref[...], head) + (
            dot_rows(rest_ref[...], head) + dot_rows(head_ref[...], rest)
        )


def one_hot_rows(count, place):
    rows = lax.broadcasted_iota(jnp.int32, (count, place.shape[1]), 0)
    return jnp.where(rows == place, 1.0, 0.0).astype(jnp.bfloat16)


def spectrum(planes, n, zh, zr, yh, yr):
    columns = []
    for i in range(0, len(planes), 2):
        pairs = planes[i : i + 2]
        rows = jnp.concatenate([jnp.concatenate(pair, axis=1) for pair in pairs], axis=0)
        rows = times_constant(rows, zh, zr)
        columns += [
            jnp.concatenate([rows[j * n : (j + 1) * n, :n], rows[j * n : (j + 1) * n, n:]], axis=0)
            for j in range(len(pairs))
        ]
    return jnp.concatenate(constant_times(yh, yr, columns), axis=1)


def ligand_kernel(place_ref, own_ref, other_ref, shape_ref, charge_ref, table_ref, zh, zr, yh, yr, out_ref):
    n = zh.shape[0] // 2
    half = n // 2
    atoms = own_ref.shape[1]
    step = pl.program_id(0)
    device = place_ref[0]
    first_half = device < table_ref.shape[0] // 2
    special = device == 0
    own, other = own_ref[pl.ds(step, 1), :], other_ref[pl.ds(step, 1), :]
    grids = []
    for cell in (jnp.where(first_half, own, other), jnp.where(first_half, other, own)):
        coord_x, coord_y, coord_z = cell // (n * n), cell // n % n, cell % n
        wave = dot(table_ref[device], one_hot_rows(n, coord_x))
        comps = wave.shape[0] // 4
        wave = wave[:comps] + (wave[comps : 2 * comps] + wave[2 * comps : 3 * comps])
        values = jnp.concatenate([wave * shape_ref[...], wave * charge_ref[...]], axis=0)
        comps = values.shape[0]
        head = values.astype(jnp.bfloat16).astype(jnp.float32)
        hit = lax.broadcasted_iota(jnp.int32, (half, atoms), 0) == coord_y % half
        stacked = jnp.concatenate(
            [
                jnp.where(hit, part[c : c + 1, :], 0.0).astype(jnp.bfloat16)
                for part in (head, values - head)
                for c in range(comps)
            ],
            axis=0,
        )
        total = dot_rows(stacked, one_hot_rows(2 * n, coord_z + n * (coord_y // half)))
        total = total[: comps * half] + total[comps * half :]
        grids.append(
            [
                jnp.concatenate(
                    [total[c * half : (c + 1) * half, :n], total[c * half : (c + 1) * half, n:]], axis=0
                )
                for c in range(comps)
            ]
        )
    planes = [[], []]
    for c in range(0, comps, 2):
        first, second = (grids[0][c], grids[0][c + 1]), (grids[1][c], grids[1][c + 1])
        if c % (comps // 2) == 0:
            first, second = (
                (first[0], jnp.where(special, second[0], first[1])),
                (jnp.where(special, first[1], second[0]), second[1]),
            )
        planes[0].append(first)
        planes[1].append(second)
    out_ref[0] = spectrum(planes[0] + planes[1], n, zh, zr, yh, yr)


def receptor_spectrum(special, blocks_ref, zh, zr, yh, yr, channels, y_parts, z_parts):
    n = zh.shape[0] // 2
    width = n // z_parts
    comps = blocks_ref.shape[1] // SUBLANES
    planes = []
    for channel in range(channels):
        parts = []
        for c in range(comps):
            rows = []
            for y_part in range(y_parts):
                first = (channel * y_parts + y_part) * z_parts
                pieces = [blocks_ref[first + i, c * SUBLANES : (c + 1) * SUBLANES, :] for i in range(z_parts)]
                rows += swap_groups(pieces, width)
            parts.append(jnp.concatenate(rows, axis=0))
        zero = jnp.zeros_like(parts[0])
        lone = jnp.where(special, zero, parts[1])
        planes.append((parts[0], lone))
        planes.append((jnp.where(special, parts[1], parts[0]), lone))
        for c in range(2, comps, 2):
            planes.append((parts[c], parts[c + 1]))
    return spectrum(planes, n, zh, zr, yh, yr)


def product_kernel(
    place_ref, blocks_ref, ligand_ref, zh, zr, yh, yr, out_ref, receptor_ref, *, channels, y_parts, z_parts
):
    n = zh.shape[0] // 2
    width = n // z_parts
    groups = LANES // width
    slots = ligand_ref.shape[2] // (2 * channels * n)
    special = place_ref[0] == 0

    @pl.when(pl.program_id(0) == 0)
    def _():
        receptor_ref[...] = receptor_spectrum(
            special, blocks_ref, zh, zr, yh, yr, channels, y_parts, z_parts
        )

    def receptor(channel, slot, rotation):
        at = channel * (slots + 1) + (rotation if slot == 0 else slot + 1)
        return receptor_ref[:n, at * n : (at + 1) * n], receptor_ref[n:, at * n : (at + 1) * n]

    def ligand(channel, slot, rotation):
        at = (rotation * channels + channel) * slots + slot
        return ligand_ref[0, :n, at * n : (at + 1) * n], ligand_ref[0, n:, at * n : (at + 1) * n]

    columns = []
    for rotation in range(2):
        for slot in range(slots):
            real, imag = 0.0, 0.0
            for channel in range(channels):
                fr, fi = receptor(channel, slot, rotation)
                hr, hi = ligand(channel, slot, rotation)
                real = real + (fr * hr + fi * hi)
                imag = imag + (fr * hi - fi * hr)
            columns.append(jnp.concatenate([real, imag], axis=0))
    columns = constant_times(yh, yr, columns)
    rows = jnp.concatenate([jnp.concatenate([c[:n], c[n:]], axis=1) for c in columns], axis=0)
    rows = times_constant(rows, zh, zr)
    maps = [
        [
            [rows[(rotation * slots + slot) * n : (rotation * slots + slot + 1) * n, p * n : (p + 1) * n] for p in range(2)]
            for slot in range(slots)
        ]
        for rotation in range(2)
    ]
    lone, other = maps[0][0][1], maps[1][0][0]
    maps[0][0][1] = jnp.where(special, other, lone)
    maps[1][0][0] = jnp.where(special, lone, other)
    for rotation in range(2):
        for slot in range(slots):
            for p in range(2):
                plane = maps[rotation][slot][p]
                row = (slot * 2 + p) * SUBLANES
                for y_part in range(y_parts):
                    pieces = [
                        plane[(y_part * groups + g) * SUBLANES : (y_part * groups + g + 1) * SUBLANES, :]
                        for g in range(groups)
                    ]
                    for z_part, block in enumerate(swap_groups(pieces, width)):
                        out_ref[(rotation * y_parts + y_part) * z_parts + z_part, row : row + SUBLANES, :] = block


def inverse_x_kernel(blocks_ref, head_ref, rest_ref, out_ref, best_ref, rows_ref):
    n = head_ref.shape[0]
    y_block, z_block = out_ref.shape[1:3]
    groups = LANES // z_block
    rows_ref[...] = blocks_ref[...].reshape(rows_ref.shape)
    best = None
    for row in range(SUBLANES):
        values = rows_ref[pl.ds(row, n, stride=SUBLANES), :]
        result = times_constant(values.T, head_ref, rest_ref)
        for g in range(groups):
            out_ref[0, g * SUBLANES + row] = result[g * z_block : (g + 1) * z_block, :]
        best = result if best is None else jnp.maximum(best, result)
    best_ref[pl.program_id(0)] = jnp.max(best)


def whole():
    return pl.BlockSpec(memory_space=pltpu.VMEM)


def scalars():
    return pl.BlockSpec(memory_space=pltpu.SMEM)


def component_tables(n, comps):
    matrix = forward_x_matrix(n).reshape(n // comps, comps, n)
    head, rest = split_constant(matrix)
    last = (matrix - head.astype(np.float64) - rest.astype(np.float64)).astype(jnp.bfloat16)
    return np.concatenate([head, rest, last, np.zeros_like(head)], axis=1)


def on_device(receptor_grids, ligand_cells, atom_shape, atom_charges, *, sizes):
    n = receptor_grids.shape[1]
    rots, y_parts, z_parts = (sizes[a] for a in AXES)
    devices = rots * y_parts * z_parts
    slots = n // 2 // devices
    comps = 2 * slots
    rows = comps * SUBLANES
    y_block, z_block = receptor_grids.shape[2:]
    rotations, atoms = ligand_cells.shape
    channels = 2
    f32 = jnp.float32
    matrices = split_constant(plus_matrix(n))
    matrices = [jnp.asarray(m) for m in (*matrices, *(np.ascontiguousarray(m.T) for m in matrices))]
    place = lax.axis_index(AXES).reshape(1)
    other = lax.ppermute(ligand_cells, "rot", [(i, i ^ 1) for i in range(rots)])

    components = pl.pallas_call(
        forward_x_kernel,
        out_shape=jax.ShapeDtypeStruct((n * SUBLANES, LANES), f32),
        in_specs=[whole()] * 3,
        out_specs=whole(),
        name="forward_x",
    )(jnp.transpose(receptor_grids, (0, 2, 3, 1)), *(jnp.asarray(m) for m in split_constant(forward_x_matrix(n))))
    components, other = lax.optimization_barrier((components, other))
    blocks = lax.all_to_all(components.reshape(devices, rows, LANES), AXES, 0, 0, tiled=True)

    width = 2 * slots * channels * n
    ligand = pl.pallas_call(
        ligand_kernel,
        grid=(rotations,),
        out_shape=jax.ShapeDtypeStruct((rotations, 2 * n, width), f32),
        in_specs=[scalars()] + [whole()] * 9,
        out_specs=pl.BlockSpec((1, 2 * n, width), lambda i: (i, 0, 0)),
        name="ligand",
    )(
        place,
        ligand_cells,
        other,
        atom_shape.reshape(1, atoms),
        atom_charges.reshape(1, atoms),
        jnp.asarray(component_tables(n, comps)),
        *matrices,
    )

    sent = pl.pallas_call(
        functools.partial(product_kernel, channels=channels, y_parts=y_parts, z_parts=z_parts),
        grid=(rotations,),
        out_shape=jax.ShapeDtypeStruct((devices, rotations * rows, LANES), f32),
        in_specs=[scalars(), whole(), pl.BlockSpec((1, 2 * n, width), lambda i: (i, 0, 0))] + [whole()] * 4,
        out_specs=pl.BlockSpec((devices, rows, LANES), lambda i: (0, i, 0)),
        scratch_shapes=[pltpu.VMEM((2 * n, channels * (slots + 1) * n), f32)],
        name="product",
    )(place, blocks, ligand, *matrices)
    got = lax.all_to_all(sent, AXES, 0, 0, tiled=True)

    correlation, best = pl.pallas_call(
        inverse_x_kernel,
        grid=(rotations,),
        out_shape=[
            jax.ShapeDtypeStruct((rotations, y_block, z_block, n), f32),
            jax.ShapeDtypeStruct((rotations,), f32),
        ],
        in_specs=[pl.BlockSpec((devices, rows, LANES), lambda i: (0, i, 0))] + [whole()] * 2,
        out_specs=[pl.BlockSpec((1, y_block, z_block, n), lambda i: (i, 0, 0, 0)), scalars()],
        scratch_shapes=[pltpu.VMEM((devices * rows, LANES), f32)],
        name="inverse_x",
    )(got, *(jnp.asarray(m) for m in split_constant(inverse_x_matrix(n))))
    for axis in ("py", "pz"):
        step = 1
        while step < sizes[axis]:
            best = jnp.maximum(best, lax.ppermute(best, axis, [(i, i ^ step) for i in range(sizes[axis])]))
            step *= 2
    return correlation, best


def twiddle(length, inverse):
    counter = jnp.arange(length, dtype=jnp.int32)
    phases = counter[:, None] * counter[None, :] % length
    angles = phases.astype(jnp.float32) * (2.0 * math.pi / length)
    factor = 1.0 if inverse else -1.0
    return (jnp.cos(angles), factor * jnp.sin(angles))


def transform(real_part, imag_part, pattern, inverse, n):
    cosine, sine_table = twiddle(n, inverse)
    if imag_part is None:
        return (
            jnp.einsum(pattern, real_part, cosine, precision=exact_mode),
            jnp.einsum(pattern, real_part, sine_table, precision=exact_mode),
        )
    new_real = jnp.einsum(pattern, real_part, cosine, precision=exact_mode) - jnp.einsum(
        pattern, imag_part, sine_table, precision=exact_mode
    )
    new_imag = jnp.einsum(pattern, real_part, sine_table, precision=exact_mode) + jnp.einsum(
        pattern, imag_part, cosine, precision=exact_mode
    )
    return (new_real, new_imag)


def exchange(pair, axis, split_axis, concat_axis):
    return tuple(lax.all_to_all(p, axis, split_axis=split_axis, concat_axis=concat_axis, tiled=True) for p in pair)


def on_any_device(receptor_grids, ligand_cells, atom_shape, atom_charges, *, sizes):
    n = receptor_grids.shape[1]
    planes = lax.all_gather(receptor_grids, "rot", axis=0, tiled=True)
    pair = transform(planes, None, "cxyz,xk->ckyz", False, n)
    pair = transform(*exchange(pair, "pz", 1, 3), "cxyz,zk->cxyk", False, n)
    receptor_real, receptor_imag = transform(*exchange(pair, "py", 3, 2), "cxyz,yk->cxkz", False, n)
    x_block = n // sizes["pz"]
    z_block = n // sizes["py"]
    kx_values = lax.axis_index("pz") * x_block + jnp.arange(x_block, dtype=jnp.int32)
    kz_values = lax.axis_index("py") * z_block + jnp.arange(z_block, dtype=jnp.int32)
    ky_values = jnp.arange(n, dtype=jnp.int32)
    weights = jnp.stack((atom_shape, atom_charges), 1)
    step_angle = 2.0 * math.pi / n

    def rotation_product(atom_cells):
        coord_x = atom_cells // (n * n)
        coord_y = atom_cells // n % n
        coord_z = atom_cells % n
        angle_y = (coord_y[:, None] * ky_values[None, :] % n).astype(jnp.float32) * step_angle
        cos_y = jnp.cos(angle_y)
        sin_y = jnp.sin(angle_y)
        phase_xz = (
            coord_x[:, None, None] * kx_values[None, :, None]
            + coord_z[:, None, None] * kz_values[None, None, :]
        ) % n
        angle_xz = phase_xz.astype(jnp.float32) * step_angle
        cos_xz = (weights[:, :, None, None] * jnp.cos(angle_xz)[:, None]).reshape(atom_cells.shape[0], -1)
        sin_xz = (weights[:, :, None, None] * jnp.sin(angle_xz)[:, None]).reshape(atom_cells.shape[0], -1)
        meet = functools.partial(jnp.einsum, "ay,ab->yb", precision=exact_mode)
        conj_real = (meet(cos_y, cos_xz) - meet(sin_y, sin_xz)).reshape(n, 2, x_block, z_block)
        conj_imag = (meet(cos_y, sin_xz) + meet(sin_y, cos_xz)).reshape(n, 2, x_block, z_block)
        join = functools.partial(jnp.einsum, "ycxz,cxyz->xyz", precision=exact_mode)
        product_real = join(conj_real, receptor_real) - join(conj_imag, receptor_imag)
        product_imag = join(conj_imag, receptor_real) + join(conj_real, receptor_imag)
        return (product_real, product_imag)

    product_real, product_imag = lax.map(rotation_product, ligand_cells)
    rotations = ligand_cells.shape[0]
    pair_real = product_real.reshape((rotations // 2, 2) + product_real.shape[1:])
    pair_imag = product_imag.reshape((rotations // 2, 2) + product_imag.shape[1:])
    pair = (pair_real[:, 0] - pair_imag[:, 1], pair_imag[:, 0] + pair_real[:, 1])
    pair = transform(*pair, "bxyz,yk->bxkz", True, n)
    pair = transform(*exchange(pair, "py", 2, 3), "bxyz,zk->bxyk", True, n)
    even_maps, odd_maps = transform(*exchange(pair, "pz", 3, 1), "bxyz,xk->byzk", True, n)
    stacked = jnp.stack((even_maps, odd_maps), 1)
    correlation = stacked.reshape((rotations,) + even_maps.shape[1:]) * (1.0 / (n * n * n))
    best_score = lax.pmax(jnp.max(correlation, axis=(1, 2, 3)), ("py", "pz"))
    return (correlation, best_score)


def solution(mesh):
    sizes = dict(mesh.shape)

    def run(receptor_grids, ligand_cells, atom_shape, atom_charges):
        n = receptor_grids.shape[1]
        devices = math.prod(sizes[a] for a in AXES)
        fits = (
            sizes["rot"] == 2
            and n == LANES
            and (n // 2) % devices == 0
            and (n // sizes["py"]) * (n // sizes["pz"]) == SUBLANES * LANES
            and all(sizes[a] & (sizes[a] - 1) == 0 for a in AXES)
        )
        body = functools.partial(on_device if fits else on_any_device, sizes=sizes)
        placed = (P("rot", None, "py", "pz"), P("rot", None), P(), P())
        return jax.shard_map(
            body,
            mesh=mesh,
            in_specs=placed,
            out_specs=(P("rot", "py", "pz", None), P("rot")),
            check_vma=False,
        )(receptor_grids, ligand_cells, atom_shape, atom_charges)

    return run
```

```python
import functools
import math

import jax
import jax.numpy as jnp
import numpy as np
from jax import lax
from jax.experimental import pallas as pl
from jax.experimental.pallas import tpu as pltpu
from jax.sharding import PartitionSpec as P

exact_mode = lax.Precision.HIGHEST
AXES = ("rot", "py", "pz")
LANES = 128
SUBLANES = 8
VMEM_BYTES = 48 << 20


def split_constant(matrix):
    head = np.asarray(matrix, np.float64).astype(jnp.bfloat16)
    rest = (np.asarray(matrix, np.float64) - head.astype(np.float64)).astype(jnp.bfloat16)
    return head, rest


def plus_matrix(n):
    turns = np.outer(np.arange(n), np.arange(n)) % n
    cosine, sine = np.cos(turns * (2 * np.pi / n)), np.sin(turns * (2 * np.pi / n))
    return np.block([[cosine, sine], [-sine, cosine]])


def component_phases(n):
    places = np.arange(n)
    phases = np.zeros((n, n), np.int64)
    for slot in range(n // 2):
        phases[2 * slot] = slot * places % n
        phases[2 * slot + 1] = (n // 2) * places % n if slot == 0 else (slot * places - n // 4) % n
    return phases


def forward_x_matrix(n):
    return np.cos(component_phases(n) * (2 * np.pi / n))


def inverse_x_matrix(n):
    matrix = np.cos(component_phases(n) * (2 * np.pi / n))
    scale = np.full((n, 1), 2.0)
    scale[3::2] = -2.0
    scale[:2] = 1.0
    return matrix * scale / float(n) ** 3


def split(value):
    head = value.astype(jnp.bfloat16)
    rest = (value - head.astype(jnp.float32)).astype(jnp.bfloat16)
    return head, rest


def dot(a, b):
    return jnp.dot(a, b, preferred_element_type=jnp.float32)


def dot_rows(a, b):
    return lax.dot_general(a, b, (((1,), (1,)), ((), ())), preferred_element_type=jnp.float32)


def times_constant(value, head_ref, rest_ref):
    head, rest = split(value)
    return dot(head, head_ref[...]) + (dot(head, rest_ref[...]) + dot(rest, head_ref[...]))


def constant_times(head_ref, rest_ref, values):
    results = []
    for i in range(0, len(values), 2):
        pair = values[i : i + 2]
        head, rest = split(jnp.concatenate(pair, axis=1))
        result = dot(head_ref[...], head) + (dot(rest_ref[...], head) + dot(head_ref[...], rest))
        width = pair[0].shape[1]
        results += [result[:, j * width : (j + 1) * width] for j in range(len(pair))]
    return results


def swap_groups(pieces, width):
    pieces = list(pieces)
    lane = lax.broadcasted_iota(jnp.int32, pieces[0].shape, 1)
    bit = len(pieces) // 2
    while bit:
        low = lane // (bit * width) % 2 == 0
        for i in range(len(pieces)):
            if i & bit == 0:
                first, second = pieces[i], pieces[i | bit]
                pieces[i] = jnp.where(low, first, pltpu.roll(second, bit * width, 1))
                pieces[i | bit] = jnp.where(low, pltpu.roll(first, LANES - bit * width, 1), second)
        bit //= 2
    return pieces


def forward_x_kernel(grid_ref, head_ref, rest_ref, out_ref):
    y_block, z_block, n = grid_ref.shape[1:]
    groups = LANES // z_block
    high = y_block // groups
    for row in range(high):
        values = jnp.concatenate([grid_ref[0, g * high + row] for g in range(groups)], axis=0)
        head, rest = split(values)
        out_ref[pl.ds(row, n, stride=high), :] = dot_rows(head_ref[...], head) + (
            dot_rows(rest_ref[...], head) + dot_rows(head_ref[...], rest)
        )


def one_hot_rows(count, place):
    rows = lax.broadcasted_iota(jnp.int32, (count, place.shape[1]), 0)
    return jnp.where(rows == place, 1.0, 0.0).astype(jnp.bfloat16)


def spectrum(planes, n, zh, zr, yh, yr):
    columns = []
    for i in range(0, len(planes), 2):
        pairs = planes[i : i + 2]
        rows = jnp.concatenate([jnp.concatenate(pair, axis=1) for pair in pairs], axis=0)
        rows = times_constant(rows, zh, zr)
        columns += [
            jnp.concatenate([rows[j * n : (j + 1) * n, :n], rows[j * n : (j + 1) * n, n:]], axis=0)
            for j in range(len(pairs))
        ]
    return jnp.concatenate(constant_times(yh, yr, columns), axis=1)


def ligand_kernel(place_ref, own_ref, other_ref, shape_ref, charge_ref, table_ref, zh, zr, yh, yr, out_ref, held_ref, sems):
    n = zh.shape[0] // 2
    half = n // 2
    atoms = own_ref.shape[1]
    step = pl.program_id(0)
    device = place_ref[0]
    first_half = device < table_ref.shape[0] // 2
    special = device == 0
    own, other = own_ref[pl.ds(step, 1), :], other_ref[pl.ds(step, 1), :]
    grids = []
    for cell in (jnp.where(first_half, own, other), jnp.where(first_half, other, own)):
        coord_x, coord_y, coord_z = cell // (n * n), cell // n % n, cell % n
        wave = dot(table_ref[device], one_hot_rows(n, coord_x))
        comps = wave.shape[0] // 4
        wave = wave[:comps] + (wave[comps : 2 * comps] + wave[2 * comps : 3 * comps])
        values = jnp.concatenate([wave * shape_ref[...], wave * charge_ref[...]], axis=0)
        comps = values.shape[0]
        head = values.astype(jnp.bfloat16).astype(jnp.float32)
        hit = lax.broadcasted_iota(jnp.int32, (half, atoms), 0) == coord_y % half
        stacked = jnp.concatenate(
            [
                jnp.where(hit, part[c : c + 1, :], 0.0).astype(jnp.bfloat16)
                for part in (head, values - head)
                for c in range(comps)
            ],
            axis=0,
        )
        total = dot_rows(stacked, one_hot_rows(2 * n, coord_z + n * (coord_y // half)))
        total = total[: comps * half] + total[comps * half :]
        grids.append(
            [
                jnp.concatenate(
                    [total[c * half : (c + 1) * half, :n], total[c * half : (c + 1) * half, n:]], axis=0
                )
                for c in range(comps)
            ]
        )
    planes = [[], []]
    for c in range(0, comps, 2):
        first, second = (grids[0][c], grids[0][c + 1]), (grids[1][c], grids[1][c + 1])
        if c % (comps // 2) == 0:
            first, second = (
                (first[0], jnp.where(special, second[0], first[1])),
                (jnp.where(special, first[1], second[0]), second[1]),
            )
        planes[0].append(first)
        planes[1].append(second)
    held_ref[step] = spectrum(planes[0] + planes[1], n, zh, zr, yh, yr)
    pltpu.make_async_copy(held_ref.at[step], out_ref.at[step], sems.at[step]).start()

    @pl.when(step == pl.num_programs(0) - 1)
    def _():
        for i in range(held_ref.shape[0]):
            pltpu.make_async_copy(held_ref.at[i], out_ref.at[i], sems.at[i]).wait()


def receptor_spectrum(special, blocks_ref, zh, zr, yh, yr, channels, y_parts, z_parts):
    n = zh.shape[0] // 2
    width = n // z_parts
    comps = blocks_ref.shape[1] // SUBLANES
    planes = []
    for channel in range(channels):
        parts = []
        for c in range(comps):
            rows = []
            for y_part in range(y_parts):
                first = (channel * y_parts + y_part) * z_parts
                pieces = [blocks_ref[first + i, c * SUBLANES : (c + 1) * SUBLANES, :] for i in range(z_parts)]
                rows += swap_groups(pieces, width)
            parts.append(jnp.concatenate(rows, axis=0))
        zero = jnp.zeros_like(parts[0])
        lone = jnp.where(special, zero, parts[1])
        planes.append((parts[0], lone))
        planes.append((jnp.where(special, parts[1], parts[0]), lone))
        for c in range(2, comps, 2):
            planes.append((parts[c], parts[c + 1]))
    return spectrum(planes, n, zh, zr, yh, yr)


def product_kernel(
    place_ref, blocks_ref, far_ref, zh, zr, yh, yr, out_ref, receptor_ref, ligand_ref, sems, *, channels, y_parts, z_parts
):
    n = zh.shape[0] // 2
    width = n // z_parts
    groups = LANES // width
    slots = ligand_ref.shape[2] // (2 * channels * n)
    special = place_ref[0] == 0
    step = pl.program_id(0)

    @pl.when(step == 0)
    def _():
        for i in range(ligand_ref.shape[0]):
            pltpu.make_async_copy(far_ref.at[i], ligand_ref.at[i], sems.at[i]).start()
        receptor_ref[...] = receptor_spectrum(
            special, blocks_ref, zh, zr, yh, yr, channels, y_parts, z_parts
        )

    pltpu.make_async_copy(far_ref.at[step], ligand_ref.at[step], sems.at[step]).wait()

    def receptor(channel, slot, rotation):
        at = channel * (slots + 1) + (rotation if slot == 0 else slot + 1)
        return receptor_ref[:n, at * n : (at + 1) * n], receptor_ref[n:, at * n : (at + 1) * n]

    def ligand(channel, slot, rotation):
        at = (rotation * channels + channel) * slots + slot
        return ligand_ref[step, :n, at * n : (at + 1) * n], ligand_ref[step, n:, at * n : (at + 1) * n]

    columns = []
    for rotation in range(2):
        for slot in range(slots):
            real, imag = 0.0, 0.0
            for channel in range(channels):
                fr, fi = receptor(channel, slot, rotation)
                hr, hi = ligand(channel, slot, rotation)
                real = real + (fr * hr + fi * hi)
                imag = imag + (fr * hi - fi * hr)
            columns.append(jnp.concatenate([real, imag], axis=0))
    columns = constant_times(yh, yr, columns)
    rows = jnp.concatenate([jnp.concatenate([c[:n], c[n:]], axis=1) for c in columns], axis=0)
    rows = times_constant(rows, zh, zr)
    maps = [
        [
            [rows[(rotation * slots + slot) * n : (rotation * slots + slot + 1) * n, p * n : (p + 1) * n] for p in range(2)]
            for slot in range(slots)
        ]
        for rotation in range(2)
    ]
    lone, other = maps[0][0][1], maps[1][0][0]
    maps[0][0][1] = jnp.where(special, other, lone)
    maps[1][0][0] = jnp.where(special, lone, other)
    for rotation in range(2):
        for slot in range(slots):
            for p in range(2):
                plane = maps[rotation][slot][p]
                row = (slot * 2 + p) * SUBLANES
                for y_part in range(y_parts):
                    pieces = [
                        plane[(y_part * groups + g) * SUBLANES : (y_part * groups + g + 1) * SUBLANES, :]
                        for g in range(groups)
                    ]
                    for z_part, block in enumerate(swap_groups(pieces, width)):
                        out_ref[(rotation * y_parts + y_part) * z_parts + z_part, row : row + SUBLANES, :] = block


def inverse_x_kernel(blocks_ref, head_ref, rest_ref, out_ref, best_ref, rows_ref):
    n = head_ref.shape[0]
    y_block, z_block = out_ref.shape[1:3]
    groups = LANES // z_block
    rows_ref[...] = blocks_ref[...].reshape(rows_ref.shape)
    best = None
    for row in range(SUBLANES):
        values = rows_ref[pl.ds(row, n, stride=SUBLANES), :]
        result = times_constant(values.T, head_ref, rest_ref)
        for g in range(groups):
            out_ref[0, g * SUBLANES + row] = result[g * z_block : (g + 1) * z_block, :]
        best = result if best is None else jnp.maximum(best, result)
    best_ref[pl.program_id(0)] = jnp.max(best)


def whole():
    return pl.BlockSpec(memory_space=pltpu.VMEM)


def room(mebibytes):
    return pltpu.CompilerParams(vmem_limit_bytes=mebibytes << 20)


def far():
    return pl.BlockSpec(memory_space=pltpu.HBM)


def scalars():
    return pl.BlockSpec(memory_space=pltpu.SMEM)


def component_tables(n, comps):
    matrix = forward_x_matrix(n).reshape(n // comps, comps, n)
    head, rest = split_constant(matrix)
    last = (matrix - head.astype(np.float64) - rest.astype(np.float64)).astype(jnp.bfloat16)
    return np.concatenate([head, rest, last, np.zeros_like(head)], axis=1)


def on_device(receptor_grids, ligand_cells, atom_shape, atom_charges, *, sizes):
    n = receptor_grids.shape[1]
    rots, y_parts, z_parts = (sizes[a] for a in AXES)
    devices = rots * y_parts * z_parts
    slots = n // 2 // devices
    comps = 2 * slots
    rows = comps * SUBLANES
    y_block, z_block = receptor_grids.shape[2:]
    rotations, atoms = ligand_cells.shape
    channels = 2
    f32 = jnp.float32
    matrices = split_constant(plus_matrix(n))
    matrices = [jnp.asarray(m) for m in (*matrices, *(np.ascontiguousarray(m.T) for m in matrices))]
    place = lax.axis_index(AXES).reshape(1)
    other = lax.ppermute(ligand_cells, "rot", [(i, i ^ 1) for i in range(rots)])

    components = pl.pallas_call(
        forward_x_kernel,
        out_shape=jax.ShapeDtypeStruct((n * SUBLANES, LANES), f32),
        in_specs=[whole()] * 3,
        out_specs=whole(),
        compiler_params=room(60),
        name="forward_x",
    )(jnp.transpose(receptor_grids, (0, 2, 3, 1)), *(jnp.asarray(m) for m in split_constant(forward_x_matrix(n))))
    components, other = lax.optimization_barrier((components, other))
    blocks = lax.all_to_all(components.reshape(devices, rows, LANES), AXES, 0, 0, tiled=True)

    width = 2 * slots * channels * n
    slabs = max(rotations, VMEM_BYTES // (2 * n * width * 4))
    ligand = pl.pallas_call(
        ligand_kernel,
        grid=(rotations,),
        out_shape=jax.ShapeDtypeStruct((slabs, 2 * n, width), f32),
        in_specs=[scalars()] + [whole()] * 9,
        out_specs=far(),
        scratch_shapes=[pltpu.VMEM((rotations, 2 * n, width), f32), pltpu.SemaphoreType.DMA((rotations,))],
        compiler_params=room(24),
        name="ligand",
    )(
        place,
        ligand_cells,
        other,
        atom_shape.reshape(1, atoms),
        atom_charges.reshape(1, atoms),
        jnp.asarray(component_tables(n, comps)),
        *matrices,
    )

    sent = pl.pallas_call(
        functools.partial(product_kernel, channels=channels, y_parts=y_parts, z_parts=z_parts),
        grid=(rotations,),
        out_shape=jax.ShapeDtypeStruct((devices, rotations * rows, LANES), f32),
        in_specs=[scalars(), whole(), far()] + [whole()] * 4,
        out_specs=pl.BlockSpec((devices, rows, LANES), lambda i: (0, i, 0)),
        scratch_shapes=[
            pltpu.VMEM((2 * n, channels * (slots + 1) * n), f32),
            pltpu.VMEM((rotations, 2 * n, width), f32),
            pltpu.SemaphoreType.DMA((rotations,)),
        ],
        compiler_params=room(16),
        name="product",
    )(place, blocks, ligand, *matrices)
    got = lax.all_to_all(sent, AXES, 0, 0, tiled=True)

    correlation, best = pl.pallas_call(
        inverse_x_kernel,
        grid=(rotations,),
        out_shape=[
            jax.ShapeDtypeStruct((rotations, y_block, z_block, n), f32),
            jax.ShapeDtypeStruct((rotations,), f32),
        ],
        in_specs=[pl.BlockSpec((devices, rows, LANES), lambda i: (0, i, 0))] + [whole()] * 2,
        out_specs=[pl.BlockSpec((1, y_block, z_block, n), lambda i: (i, 0, 0, 0)), scalars()],
        scratch_shapes=[pltpu.VMEM((devices * rows, LANES), f32)],
        compiler_params=room(8),
        name="inverse_x",
    )(got, *(jnp.asarray(m) for m in split_constant(inverse_x_matrix(n))))
    for axis in ("py", "pz"):
        step = 1
        while step < sizes[axis]:
            best = jnp.maximum(best, lax.ppermute(best, axis, [(i, i ^ step) for i in range(sizes[axis])]))
            step *= 2
    return correlation, best


def twiddle(length, inverse):
    counter = jnp.arange(length, dtype=jnp.int32)
    phases = counter[:, None] * counter[None, :] % length
    angles = phases.astype(jnp.float32) * (2.0 * math.pi / length)
    factor = 1.0 if inverse else -1.0
    return (jnp.cos(angles), factor * jnp.sin(angles))


def transform(real_part, imag_part, pattern, inverse, n):
    cosine, sine_table = twiddle(n, inverse)
    if imag_part is None:
        return (
            jnp.einsum(pattern, real_part, cosine, precision=exact_mode),
            jnp.einsum(pattern, real_part, sine_table, precision=exact_mode),
        )
    new_real = jnp.einsum(pattern, real_part, cosine, precision=exact_mode) - jnp.einsum(
        pattern, imag_part, sine_table, precision=exact_mode
    )
    new_imag = jnp.einsum(pattern, real_part, sine_table, precision=exact_mode) + jnp.einsum(
        pattern, imag_part, cosine, precision=exact_mode
    )
    return (new_real, new_imag)


def exchange(pair, axis, split_axis, concat_axis):
    return tuple(lax.all_to_all(p, axis, split_axis=split_axis, concat_axis=concat_axis, tiled=True) for p in pair)


def on_any_device(receptor_grids, ligand_cells, atom_shape, atom_charges, *, sizes):
    n = receptor_grids.shape[1]
    planes = lax.all_gather(receptor_grids, "rot", axis=0, tiled=True)
    pair = transform(planes, None, "cxyz,xk->ckyz", False, n)
    pair = transform(*exchange(pair, "pz", 1, 3), "cxyz,zk->cxyk", False, n)
    receptor_real, receptor_imag = transform(*exchange(pair, "py", 3, 2), "cxyz,yk->cxkz", False, n)
    x_block = n // sizes["pz"]
    z_block = n // sizes["py"]
    kx_values = lax.axis_index("pz") * x_block + jnp.arange(x_block, dtype=jnp.int32)
    kz_values = lax.axis_index("py") * z_block + jnp.arange(z_block, dtype=jnp.int32)
    ky_values = jnp.arange(n, dtype=jnp.int32)
    weights = jnp.stack((atom_shape, atom_charges), 1)
    step_angle = 2.0 * math.pi / n

    def rotation_product(atom_cells):
        coord_x = atom_cells // (n * n)
        coord_y = atom_cells // n % n
        coord_z = atom_cells % n
        angle_y = (coord_y[:, None] * ky_values[None, :] % n).astype(jnp.float32) * step_angle
        cos_y = jnp.cos(angle_y)
        sin_y = jnp.sin(angle_y)
        phase_xz = (
            coord_x[:, None, None] * kx_values[None, :, None]
            + coord_z[:, None, None] * kz_values[None, None, :]
        ) % n
        angle_xz = phase_xz.astype(jnp.float32) * step_angle
        cos_xz = (weights[:, :, None, None] * jnp.cos(angle_xz)[:, None]).reshape(atom_cells.shape[0], -1)
        sin_xz = (weights[:, :, None, None] * jnp.sin(angle_xz)[:, None]).reshape(atom_cells.shape[0], -1)
        meet = functools.partial(jnp.einsum, "ay,ab->yb", precision=exact_mode)
        conj_real = (meet(cos_y, cos_xz) - meet(sin_y, sin_xz)).reshape(n, 2, x_block, z_block)
        conj_imag = (meet(cos_y, sin_xz) + meet(sin_y, cos_xz)).reshape(n, 2, x_block, z_block)
        join = functools.partial(jnp.einsum, "ycxz,cxyz->xyz", precision=exact_mode)
        product_real = join(conj_real, receptor_real) - join(conj_imag, receptor_imag)
        product_imag = join(conj_imag, receptor_real) + join(conj_real, receptor_imag)
        return (product_real, product_imag)

    product_real, product_imag = lax.map(rotation_product, ligand_cells)
    rotations = ligand_cells.shape[0]
    pair_real = product_real.reshape((rotations // 2, 2) + product_real.shape[1:])
    pair_imag = product_imag.reshape((rotations // 2, 2) + product_imag.shape[1:])
    pair = (pair_real[:, 0] - pair_imag[:, 1], pair_imag[:, 0] + pair_real[:, 1])
    pair = transform(*pair, "bxyz,yk->bxkz", True, n)
    pair = transform(*exchange(pair, "py", 2, 3), "bxyz,zk->bxyk", True, n)
    even_maps, odd_maps = transform(*exchange(pair, "pz", 3, 1), "bxyz,xk->byzk", True, n)
    stacked = jnp.stack((even_maps, odd_maps), 1)
    correlation = stacked.reshape((rotations,) + even_maps.shape[1:]) * (1.0 / (n * n * n))
    best_score = lax.pmax(jnp.max(correlation, axis=(1, 2, 3)), ("py", "pz"))
    return (correlation, best_score)


def solution(mesh):
    sizes = dict(mesh.shape)

    def run(receptor_grids, ligand_cells, atom_shape, atom_charges):
        n = receptor_grids.shape[1]
        devices = math.prod(sizes[a] for a in AXES)
        fits = (
            sizes["rot"] == 2
            and n == LANES
            and (n // 2) % devices == 0
            and (n // sizes["py"]) * (n // sizes["pz"]) == SUBLANES * LANES
            and all(sizes[a] & (sizes[a] - 1) == 0 for a in AXES)
        )
        body = functools.partial(on_device if fits else on_any_device, sizes=sizes)
        placed = (P("rot", None, "py", "pz"), P("rot", None), P(), P())
        return jax.shard_map(
            body,
            mesh=mesh,
            in_specs=placed,
            out_specs=(P("rot", "py", "pz", None), P("rot")),
            check_vma=False,
        )(receptor_grids, ligand_cells, atom_shape, atom_charges)

    return run
```

```python
import functools
import math

import jax
import jax.numpy as jnp
import numpy as np
from jax import lax
from jax.experimental import pallas as pl
from jax.experimental.pallas import tpu as pltpu
from jax.sharding import PartitionSpec as P

exact_mode = lax.Precision.HIGHEST
AXES = ("rot", "py", "pz")
LANES = 128
SUBLANES = 8
VMEM_BYTES = 48 << 20


def split_constant(matrix):
    head = np.asarray(matrix, np.float64).astype(jnp.bfloat16)
    rest = (np.asarray(matrix, np.float64) - head.astype(np.float64)).astype(jnp.bfloat16)
    return head, rest


def plus_matrix(n):
    turns = np.outer(np.arange(n), np.arange(n)) % n
    cosine, sine = np.cos(turns * (2 * np.pi / n)), np.sin(turns * (2 * np.pi / n))
    return np.block([[cosine, sine], [-sine, cosine]])


def component_phases(n):
    places = np.arange(n)
    phases = np.zeros((n, n), np.int64)
    for slot in range(n // 2):
        phases[2 * slot] = slot * places % n
        phases[2 * slot + 1] = (n // 2) * places % n if slot == 0 else (slot * places - n // 4) % n
    return phases


def forward_x_matrix(n):
    return np.cos(component_phases(n) * (2 * np.pi / n))


def inverse_x_matrix(n):
    matrix = np.cos(component_phases(n) * (2 * np.pi / n))
    scale = np.full((n, 1), 2.0)
    scale[3::2] = -2.0
    scale[:2] = 1.0
    return matrix * scale / float(n) ** 3


def split(value):
    head = value.astype(jnp.bfloat16)
    rest = (value - head.astype(jnp.float32)).astype(jnp.bfloat16)
    return head, rest


def dot(a, b):
    return jnp.dot(a, b, preferred_element_type=jnp.float32)


def dot_rows(a, b):
    return lax.dot_general(a, b, (((1,), (1,)), ((), ())), preferred_element_type=jnp.float32)


def times_constant(value, head_ref, rest_ref):
    head, rest = split(value)
    return dot(head, head_ref[...]) + (dot(head, rest_ref[...]) + dot(rest, head_ref[...]))


def constant_times(head_ref, rest_ref, values):
    results = []
    for i in range(0, len(values), 2):
        pair = values[i : i + 2]
        head, rest = split(jnp.concatenate(pair, axis=1))
        result = dot(head_ref[...], head) + (dot(rest_ref[...], head) + dot(head_ref[...], rest))
        width = pair[0].shape[1]
        results += [result[:, j * width : (j + 1) * width] for j in range(len(pair))]
    return results


def swap_groups(pieces, width):
    pieces = list(pieces)
    lane = lax.broadcasted_iota(jnp.int32, pieces[0].shape, 1)
    bit = len(pieces) // 2
    while bit:
        low = lane // (bit * width) % 2 == 0
        for i in range(len(pieces)):
            if i & bit == 0:
                first, second = pieces[i], pieces[i | bit]
                pieces[i] = jnp.where(low, first, pltpu.roll(second, bit * width, 1))
                pieces[i | bit] = jnp.where(low, pltpu.roll(first, LANES - bit * width, 1), second)
        bit //= 2
    return pieces


def forward_x_kernel(grid_ref, head_ref, rest_ref, out_ref):
    y_block, z_block, n = grid_ref.shape[1:]
    groups = LANES // z_block
    high = y_block // groups
    for row in range(high):
        values = jnp.concatenate([grid_ref[0, g * high + row] for g in range(groups)], axis=0)
        head, rest = split(values)
        out_ref[pl.ds(row, n, stride=high), :] = dot_rows(head_ref[...], head) + (
            dot_rows(rest_ref[...], head) + dot_rows(head_ref[...], rest)
        )


def one_hot_rows(count, place):
    rows = lax.broadcasted_iota(jnp.int32, (count, place.shape[1]), 0)
    return jnp.where(rows == place, 1.0, 0.0).astype(jnp.bfloat16)


def spectrum(planes, n, zh, zr, yh, yr):
    columns = []
    for i in range(0, len(planes), 2):
        pairs = planes[i : i + 2]
        rows = jnp.concatenate([jnp.concatenate(pair, axis=1) for pair in pairs], axis=0)
        rows = times_constant(rows, zh, zr)
        columns += [
            jnp.concatenate([rows[j * n : (j + 1) * n, :n], rows[j * n : (j + 1) * n, n:]], axis=0)
            for j in range(len(pairs))
        ]
    return constant_times(yh, yr, columns)


def ligand_kernel(place_ref, own_ref, other_ref, shape_ref, charge_ref, table_ref, zh, zr, yh, yr, far_ref, near_ref, held_ref, sems):
    n = zh.shape[0] // 2
    half = n // 2
    atoms = own_ref.shape[1]
    step = pl.program_id(0)
    device = place_ref[0]
    first_half = device < table_ref.shape[0] // 2
    special = device == 0
    own, other = own_ref[pl.ds(step, 1), :], other_ref[pl.ds(step, 1), :]
    grids = []
    for cell in (jnp.where(first_half, own, other), jnp.where(first_half, other, own)):
        coord_x, coord_y, coord_z = cell // (n * n), cell // n % n, cell % n
        wave = dot(table_ref[device], one_hot_rows(n, coord_x))
        comps = wave.shape[0] // 4
        wave = wave[:comps] + (wave[comps : 2 * comps] + wave[2 * comps : 3 * comps])
        values = jnp.concatenate([wave * shape_ref[...], wave * charge_ref[...]], axis=0)
        comps = values.shape[0]
        head = values.astype(jnp.bfloat16).astype(jnp.float32)
        hit = lax.broadcasted_iota(jnp.int32, (half, atoms), 0) == coord_y % half
        stacked = jnp.concatenate(
            [
                jnp.where(hit, part[c : c + 1, :], 0.0).astype(jnp.bfloat16)
                for part in (head, values - head)
                for c in range(comps)
            ],
            axis=0,
        )
        total = dot_rows(stacked, one_hot_rows(2 * n, coord_z + n * (coord_y // half)))
        total = total[: comps * half] + total[comps * half :]
        grids.append(
            [
                jnp.concatenate(
                    [total[c * half : (c + 1) * half, :n], total[c * half : (c + 1) * half, n:]], axis=0
                )
                for c in range(comps)
            ]
        )
    planes = [[], []]
    for c in range(0, comps, 2):
        first, second = (grids[0][c], grids[0][c + 1]), (grids[1][c], grids[1][c + 1])
        if c % (comps // 2) == 0:
            first, second = (
                (first[0], jnp.where(special, second[0], first[1])),
                (jnp.where(special, first[1], second[0]), second[1]),
            )
        planes[0].append(first)
        planes[1].append(second)
    near_ref[...] = jnp.concatenate(spectrum(planes[0] + planes[1], n, zh, zr, yh, yr), axis=1)
    last = pl.num_programs(0) - 1

    @pl.when(step < last)
    def _():
        held_ref[step] = near_ref[...]
        pltpu.make_async_copy(held_ref.at[step], far_ref.at[step], sems.at[step]).start()

    @pl.when(step == last)
    def _():
        for i in range(held_ref.shape[0]):
            pltpu.make_async_copy(held_ref.at[i], far_ref.at[i], sems.at[i]).wait()


def receptor_spectrum(special, blocks_ref, zh, zr, yh, yr, channels, y_parts, z_parts):
    n = zh.shape[0] // 2
    width = n // z_parts
    comps = blocks_ref.shape[1] // SUBLANES
    planes = []
    for channel in range(channels):
        parts = []
        for c in range(comps):
            rows = []
            for y_part in range(y_parts):
                first = (channel * y_parts + y_part) * z_parts
                pieces = [blocks_ref[first + i, c * SUBLANES : (c + 1) * SUBLANES, :] for i in range(z_parts)]
                rows += swap_groups(pieces, width)
            parts.append(jnp.concatenate(rows, axis=0))
        zero = jnp.zeros_like(parts[0])
        lone = jnp.where(special, zero, parts[1])
        planes.append((parts[0], lone))
        planes.append((jnp.where(special, parts[1], parts[0]), lone))
        for c in range(2, comps, 2):
            planes.append((parts[c], parts[c + 1]))
    return spectrum(planes, n, zh, zr, yh, yr)


def product_kernel(
    place_ref, blocks_ref, far_ref, near_ref, zh, zr, yh, yr, out_ref, ligand_ref, sems, *, channels, y_parts, z_parts
):
    n = zh.shape[0] // 2
    width = n // z_parts
    groups = LANES // width
    slots = near_ref.shape[1] // (2 * channels * n)
    last = ligand_ref.shape[0]
    special = place_ref[0] == 0
    copies = [pltpu.make_async_copy(far_ref.at[i], ligand_ref.at[i], sems.at[i]) for i in range(last)]
    for copy in copies:
        copy.start()
    receptor = receptor_spectrum(special, blocks_ref, zh, zr, yh, yr, channels, y_parts, z_parts)
    for copy in copies:
        copy.wait()

    for step in range(last + 1):
        ligand = near_ref if step == last else ligand_ref.at[step]
        columns = []
        for rotation in range(2):
            for slot in range(slots):
                real, imag = 0.0, 0.0
                for channel in range(channels):
                    f = receptor[channel * (slots + 1) + (rotation if slot == 0 else slot + 1)]
                    at = ((rotation * channels + channel) * slots + slot) * n
                    fr, fi = f[:n], f[n:]
                    hr, hi = ligand[:n, at : at + n], ligand[n:, at : at + n]
                    real = real + (fr * hr + fi * hi)
                    imag = imag + (fr * hi - fi * hr)
                columns.append(jnp.concatenate([real, imag], axis=0))
        columns = constant_times(yh, yr, columns)
        rows = jnp.concatenate([jnp.concatenate([c[:n], c[n:]], axis=1) for c in columns], axis=0)
        rows = times_constant(rows, zh, zr)
        maps = []
        for i in range(2 * slots):
            both = rows[i * n : (i + 1) * n]
            maps += [both[:, :n], both[:, n:]]
        lone, other = maps[1], maps[2 * slots]
        maps[1], maps[2 * slots] = jnp.where(special, other, lone), jnp.where(special, lone, other)
        for i, plane in enumerate(maps):
            rotation, component = divmod(i, 2 * slots)
            row = (step * 2 * slots + component) * SUBLANES
            for y_part in range(y_parts):
                first = y_part * groups
                pieces = [plane[(first + g) * SUBLANES : (first + g + 1) * SUBLANES] for g in range(groups)]
                for z_part, block in enumerate(swap_groups(pieces, width)):
                    out_ref[(rotation * y_parts + y_part) * z_parts + z_part, row : row + SUBLANES] = block


def inverse_x_kernel(blocks_ref, head_ref, rest_ref, out_ref, best_ref, rows_ref):
    n = head_ref.shape[0]
    _, z_block = out_ref.shape[1:3]
    groups = LANES // z_block
    step = pl.program_id(0)
    count = rows_ref.shape[0] // blocks_ref.shape[0]
    first = pl.multiple_of(step * count, SUBLANES)
    rows_ref[...] = blocks_ref[:, pl.ds(first, count), :].reshape(rows_ref.shape)
    best = None
    for row in range(SUBLANES):
        values = rows_ref[pl.ds(row, n, stride=SUBLANES), :]
        result = times_constant(values.T, head_ref, rest_ref)
        for g in range(groups):
            out_ref[0, g * SUBLANES + row] = result[g * z_block : (g + 1) * z_block, :]
        best = result if best is None else jnp.maximum(best, result)
    best_ref[step] = jnp.max(best)


def whole():
    return pl.BlockSpec(memory_space=pltpu.VMEM)


def room(mebibytes):
    return pltpu.CompilerParams(vmem_limit_bytes=mebibytes << 20)


def far():
    return pl.BlockSpec(memory_space=pltpu.HBM)


def scalars():
    return pl.BlockSpec(memory_space=pltpu.SMEM)


def component_tables(n, comps):
    matrix = forward_x_matrix(n).reshape(n // comps, comps, n)
    head, rest = split_constant(matrix)
    last = (matrix - head.astype(np.float64) - rest.astype(np.float64)).astype(jnp.bfloat16)
    return np.concatenate([head, rest, last, np.zeros_like(head)], axis=1)


def on_device(receptor_grids, ligand_cells, atom_shape, atom_charges, *, sizes):
    n = receptor_grids.shape[1]
    rots, y_parts, z_parts = (sizes[a] for a in AXES)
    devices = rots * y_parts * z_parts
    slots = n // 2 // devices
    comps = 2 * slots
    rows = comps * SUBLANES
    y_block, z_block = receptor_grids.shape[2:]
    rotations, atoms = ligand_cells.shape
    channels = 2
    f32 = jnp.float32
    matrices = split_constant(plus_matrix(n))
    matrices = [jnp.asarray(m) for m in (*matrices, *(np.ascontiguousarray(m.T) for m in matrices))]
    place = lax.axis_index(AXES).reshape(1)

    components = pl.pallas_call(
        forward_x_kernel,
        out_shape=jax.ShapeDtypeStruct((n * SUBLANES, LANES), f32),
        in_specs=[whole()] * 3,
        out_specs=whole(),
        compiler_params=room(60),
        name="forward_x",
    )(jnp.transpose(receptor_grids, (0, 2, 3, 1)), *(jnp.asarray(m) for m in split_constant(forward_x_matrix(n))))
    components, cells = lax.optimization_barrier((components, ligand_cells))
    other = lax.ppermute(cells, "rot", [(i, i ^ 1) for i in range(rots)])
    blocks = lax.all_to_all(components.reshape(devices, rows, LANES), AXES, 0, 0, tiled=True)

    width = 2 * slots * channels * n
    slabs = max(rotations, VMEM_BYTES // (2 * n * width * 4))
    far_ligand, near_ligand = pl.pallas_call(
        ligand_kernel,
        grid=(rotations,),
        out_shape=[
            jax.ShapeDtypeStruct((slabs, 2 * n, width), f32),
            jax.ShapeDtypeStruct((2 * n, width), f32),
        ],
        in_specs=[scalars()] + [whole()] * 9,
        out_specs=[far(), whole()],
        scratch_shapes=[pltpu.VMEM((rotations - 1, 2 * n, width), f32), pltpu.SemaphoreType.DMA((rotations - 1,))],
        compiler_params=room(24),
        name="ligand",
    )(
        place,
        ligand_cells,
        other,
        atom_shape.reshape(1, atoms),
        atom_charges.reshape(1, atoms),
        jnp.asarray(component_tables(n, comps)),
        *matrices,
    )

    sent = pl.pallas_call(
        functools.partial(product_kernel, channels=channels, y_parts=y_parts, z_parts=z_parts),
        out_shape=jax.ShapeDtypeStruct((devices, rotations * rows, LANES), f32),
        in_specs=[scalars(), whole(), far()] + [whole()] * 5,
        out_specs=whole(),
        scratch_shapes=[pltpu.VMEM((rotations - 1, 2 * n, width), f32), pltpu.SemaphoreType.DMA((rotations - 1,))],
        compiler_params=room(16),
        name="product",
    )(place, blocks, far_ligand, near_ligand, *matrices)
    got = lax.all_to_all(sent, AXES, 0, 0, tiled=True)

    correlation, best = pl.pallas_call(
        inverse_x_kernel,
        grid=(rotations,),
        out_shape=[
            jax.ShapeDtypeStruct((rotations, y_block, z_block, n), f32),
            jax.ShapeDtypeStruct((rotations,), f32),
        ],
        in_specs=[whole()] * 3,
        out_specs=[pl.BlockSpec((1, y_block, z_block, n), lambda i: (i, 0, 0, 0)), scalars()],
        scratch_shapes=[pltpu.VMEM((devices * rows, LANES), f32)],
        compiler_params=room(8),
        name="inverse_x",
    )(got, *(jnp.asarray(m) for m in split_constant(inverse_x_matrix(n))))
    for axis in ("py", "pz"):
        step = 1
        while step < sizes[axis]:
            best = jnp.maximum(best, lax.ppermute(best, axis, [(i, i ^ step) for i in range(sizes[axis])]))
            step *= 2
    return correlation, best


def twiddle(length, inverse):
    counter = jnp.arange(length, dtype=jnp.int32)
    phases = counter[:, None] * counter[None, :] % length
    angles = phases.astype(jnp.float32) * (2.0 * math.pi / length)
    factor = 1.0 if inverse else -1.0
    return (jnp.cos(angles), factor * jnp.sin(angles))


def transform(real_part, imag_part, pattern, inverse, n):
    cosine, sine_table = twiddle(n, inverse)
    if imag_part is None:
        return (
            jnp.einsum(pattern, real_part, cosine, precision=exact_mode),
            jnp.einsum(pattern, real_part, sine_table, precision=exact_mode),
        )
    new_real = jnp.einsum(pattern, real_part, cosine, precision=exact_mode) - jnp.einsum(
        pattern, imag_part, sine_table, precision=exact_mode
    )
    new_imag = jnp.einsum(pattern, real_part, sine_table, precision=exact_mode) + jnp.einsum(
        pattern, imag_part, cosine, precision=exact_mode
    )
    return (new_real, new_imag)


def exchange(pair, axis, split_axis, concat_axis):
    return tuple(lax.all_to_all(p, axis, split_axis=split_axis, concat_axis=concat_axis, tiled=True) for p in pair)


def on_any_device(receptor_grids, ligand_cells, atom_shape, atom_charges, *, sizes):
    n = receptor_grids.shape[1]
    planes = lax.all_gather(receptor_grids, "rot", axis=0, tiled=True)
    pair = transform(planes, None, "cxyz,xk->ckyz", False, n)
    pair = transform(*exchange(pair, "pz", 1, 3), "cxyz,zk->cxyk", False, n)
    receptor_real, receptor_imag = transform(*exchange(pair, "py", 3, 2), "cxyz,yk->cxkz", False, n)
    x_block = n // sizes["pz"]
    z_block = n // sizes["py"]
    kx_values = lax.axis_index("pz") * x_block + jnp.arange(x_block, dtype=jnp.int32)
    kz_values = lax.axis_index("py") * z_block + jnp.arange(z_block, dtype=jnp.int32)
    ky_values = jnp.arange(n, dtype=jnp.int32)
    weights = jnp.stack((atom_shape, atom_charges), 1)
    step_angle = 2.0 * math.pi / n

    def rotation_product(atom_cells):
        coord_x = atom_cells // (n * n)
        coord_y = atom_cells // n % n
        coord_z = atom_cells % n
        angle_y = (coord_y[:, None] * ky_values[None, :] % n).astype(jnp.float32) * step_angle
        cos_y = jnp.cos(angle_y)
        sin_y = jnp.sin(angle_y)
        phase_xz = (
            coord_x[:, None, None] * kx_values[None, :, None]
            + coord_z[:, None, None] * kz_values[None, None, :]
        ) % n
        angle_xz = phase_xz.astype(jnp.float32) * step_angle
        cos_xz = (weights[:, :, None, None] * jnp.cos(angle_xz)[:, None]).reshape(atom_cells.shape[0], -1)
        sin_xz = (weights[:, :, None, None] * jnp.sin(angle_xz)[:, None]).reshape(atom_cells.shape[0], -1)
        meet = functools.partial(jnp.einsum, "ay,ab->yb", precision=exact_mode)
        conj_real = (meet(cos_y, cos_xz) - meet(sin_y, sin_xz)).reshape(n, 2, x_block, z_block)
        conj_imag = (meet(cos_y, sin_xz) + meet(sin_y, cos_xz)).reshape(n, 2, x_block, z_block)
        join = functools.partial(jnp.einsum, "ycxz,cxyz->xyz", precision=exact_mode)
        product_real = join(conj_real, receptor_real) - join(conj_imag, receptor_imag)
        product_imag = join(conj_imag, receptor_real) + join(conj_real, receptor_imag)
        return (product_real, product_imag)

    product_real, product_imag = lax.map(rotation_product, ligand_cells)
    rotations = ligand_cells.shape[0]
    pair_real = product_real.reshape((rotations // 2, 2) + product_real.shape[1:])
    pair_imag = product_imag.reshape((rotations // 2, 2) + product_imag.shape[1:])
    pair = (pair_real[:, 0] - pair_imag[:, 1], pair_imag[:, 0] + pair_real[:, 1])
    pair = transform(*pair, "bxyz,yk->bxkz", True, n)
    pair = transform(*exchange(pair, "py", 2, 3), "bxyz,zk->bxyk", True, n)
    even_maps, odd_maps = transform(*exchange(pair, "pz", 3, 1), "bxyz,xk->byzk", True, n)
    stacked = jnp.stack((even_maps, odd_maps), 1)
    correlation = stacked.reshape((rotations,) + even_maps.shape[1:]) * (1.0 / (n * n * n))
    best_score = lax.pmax(jnp.max(correlation, axis=(1, 2, 3)), ("py", "pz"))
    return (correlation, best_score)


def solution(mesh):
    sizes = dict(mesh.shape)
    placed = (P("rot", None, "py", "pz"), P("rot", None), P(), P())

    def run(receptor_grids, ligand_cells, atom_shape, atom_charges):
        n = receptor_grids.shape[1]
        devices = math.prod(sizes[a] for a in AXES)
        fits = (
            sizes["rot"] == 2
            and n == LANES
            and (n // 2) % devices == 0
            and (n // sizes["py"]) * (n // sizes["pz"]) == SUBLANES * LANES
            and all(sizes[a] & (sizes[a] - 1) == 0 for a in AXES)
        )
        step = jax.shard_map(
            functools.partial(on_device if fits else on_any_device, sizes=sizes),
            mesh=mesh,
            in_specs=placed,
            out_specs=(P("rot", "py", "pz", None), P("rot")),
            check_vma=False,
        )
        return step(receptor_grids, ligand_cells, atom_shape, atom_charges)

    return run
```

```python
import functools
import math

import jax
import jax.numpy as jnp
import numpy as np
from jax import lax
from jax.experimental import pallas as pl
from jax.experimental.pallas import tpu as pltpu
from jax.sharding import PartitionSpec as P

exact_mode = lax.Precision.HIGHEST
AXES = ("rot", "py", "pz")
LANES = 128
SUBLANES = 8
VMEM_BYTES = 48 << 20


def split_constant(matrix):
    head = np.asarray(matrix, np.float64).astype(jnp.bfloat16)
    rest = (np.asarray(matrix, np.float64) - head.astype(np.float64)).astype(jnp.bfloat16)
    return head, rest


def plus_matrix(n):
    turns = np.outer(np.arange(n), np.arange(n)) % n
    cosine, sine = np.cos(turns * (2 * np.pi / n)), np.sin(turns * (2 * np.pi / n))
    return np.block([[cosine, sine], [-sine, cosine]])


def component_phases(n):
    places = np.arange(n)
    phases = np.zeros((n, n), np.int64)
    for slot in range(n // 2):
        phases[2 * slot] = slot * places % n
        phases[2 * slot + 1] = (n // 2) * places % n if slot == 0 else (slot * places - n // 4) % n
    return phases


def forward_x_matrix(n):
    return np.cos(component_phases(n) * (2 * np.pi / n))


def inverse_x_matrix(n):
    matrix = np.cos(component_phases(n) * (2 * np.pi / n))
    scale = np.full((n, 1), 2.0)
    scale[3::2] = -2.0
    scale[:2] = 1.0
    return matrix * scale / float(n) ** 3


def split(value):
    head = value.astype(jnp.bfloat16)
    rest = (value - head.astype(jnp.float32)).astype(jnp.bfloat16)
    return head, rest


def dot(a, b):
    return jnp.dot(a, b, preferred_element_type=jnp.float32)


def dot_rows(a, b):
    return lax.dot_general(a, b, (((1,), (1,)), ((), ())), preferred_element_type=jnp.float32)


def times_constant(value, head_ref, rest_ref):
    head, rest = split(value)
    count = value.shape[0]
    both = dot(jnp.concatenate([head, rest], axis=0), head_ref[...])
    return both[:count] + (dot(head, rest_ref[...]) + both[count:])


def constant_times(both_ref, values):
    count = both_ref.shape[0] // 2
    results = []
    for i in range(0, len(values), 2):
        pair = values[i : i + 2]
        head, rest = split(jnp.concatenate(pair, axis=1))
        both = dot(both_ref[...], head)
        result = both[:count] + (both[count:] + dot(both_ref[:count], rest))
        width = pair[0].shape[1]
        results += [result[:, j * width : (j + 1) * width] for j in range(len(pair))]
    return results


def swap_groups(pieces, width):
    pieces = list(pieces)
    lane = lax.broadcasted_iota(jnp.int32, pieces[0].shape, 1)
    bit = len(pieces) // 2
    while bit:
        low = lane // (bit * width) % 2 == 0
        for i in range(len(pieces)):
            if i & bit == 0:
                first, second = pieces[i], pieces[i | bit]
                pieces[i] = jnp.where(low, first, pltpu.roll(second, bit * width, 1))
                pieces[i | bit] = jnp.where(low, pltpu.roll(first, LANES - bit * width, 1), second)
        bit //= 2
    return pieces


def forward_x_kernel(grid_ref, head_ref, rest_ref, out_ref):
    y_block, z_block, n = grid_ref.shape[1:]
    groups = LANES // z_block
    high = y_block // groups
    for row in range(high):
        values = jnp.concatenate([grid_ref[0, g * high + row] for g in range(groups)], axis=0)
        head, rest = split(values)
        out_ref[pl.ds(row, n, stride=high), :] = dot_rows(head_ref[...], head) + (
            dot_rows(rest_ref[...], head) + dot_rows(head_ref[...], rest)
        )


def one_hot_rows(count, place):
    rows = lax.broadcasted_iota(jnp.int32, (count, place.shape[1]), 0)
    return jnp.where(rows == place, 1.0, 0.0).astype(jnp.bfloat16)


def spectrum(planes, n, zh, zr, yb, at_once):
    columns = []
    for i in range(0, len(planes), at_once):
        pairs = planes[i : i + at_once]
        rows = jnp.concatenate([jnp.concatenate(pair, axis=1) for pair in pairs], axis=0)
        rows = times_constant(rows, zh, zr)
        columns += [
            jnp.concatenate([rows[j * n : (j + 1) * n, :n], rows[j * n : (j + 1) * n, n:]], axis=0)
            for j in range(len(pairs))
        ]
    return constant_times(yb, columns)


def ligand_kernel(place_ref, own_ref, other_ref, shape_ref, charge_ref, table_ref, zh, zr, yb, far_ref, near_ref, held_ref, sems):
    n = zh.shape[0] // 2
    half = n // 2
    atoms = own_ref.shape[1]
    step = pl.program_id(0)
    device = place_ref[0]
    first_half = device < table_ref.shape[0] // 2
    special = device == 0
    own, other = own_ref[pl.ds(step, 1), :], other_ref[pl.ds(step, 1), :]
    grids = []
    for cell in (jnp.where(first_half, own, other), jnp.where(first_half, other, own)):
        coord_x, coord_y, coord_z = cell // (n * n), cell // n % n, cell % n
        wave = dot(table_ref[device], one_hot_rows(n, coord_x))
        comps = wave.shape[0] // 4
        wave = wave[:comps] + (wave[comps : 2 * comps] + wave[2 * comps : 3 * comps])
        values = jnp.concatenate([wave * shape_ref[...], wave * charge_ref[...]], axis=0)
        comps = values.shape[0]
        head = values.astype(jnp.bfloat16).astype(jnp.float32)
        hit = lax.broadcasted_iota(jnp.int32, (half, atoms), 0) == coord_y % half
        stacked = jnp.concatenate(
            [
                jnp.where(hit, part[c : c + 1, :], 0.0).astype(jnp.bfloat16)
                for part in (head, values - head)
                for c in range(comps)
            ],
            axis=0,
        )
        total = dot_rows(stacked, one_hot_rows(2 * n, coord_z + n * (coord_y // half)))
        total = total[: comps * half] + total[comps * half :]
        grids.append(
            [
                jnp.concatenate(
                    [total[c * half : (c + 1) * half, :n], total[c * half : (c + 1) * half, n:]], axis=0
                )
                for c in range(comps)
            ]
        )
    planes = [[], []]
    for c in range(0, comps, 2):
        first, second = (grids[0][c], grids[0][c + 1]), (grids[1][c], grids[1][c + 1])
        if c % (comps // 2) == 0:
            first, second = (
                (first[0], jnp.where(special, second[0], first[1])),
                (jnp.where(special, first[1], second[0]), second[1]),
            )
        planes[0].append(first)
        planes[1].append(second)
    near_ref[...] = jnp.concatenate(spectrum(planes[0] + planes[1], n, zh, zr, yb, 2), axis=1)
    last = pl.num_programs(0) - 1

    @pl.when(step < last)
    def _():
        held_ref[step] = near_ref[...]
        pltpu.make_async_copy(held_ref.at[step], far_ref.at[step], sems.at[step]).start()

    @pl.when(step == last)
    def _():
        for i in range(held_ref.shape[0]):
            pltpu.make_async_copy(held_ref.at[i], far_ref.at[i], sems.at[i]).wait()


def receptor_spectrum(special, blocks_ref, zh, zr, yb, channels, y_parts, z_parts):
    n = zh.shape[0] // 2
    width = n // z_parts
    comps = blocks_ref.shape[1] // SUBLANES
    planes = []
    for channel in range(channels):
        parts = []
        for c in range(comps):
            rows = []
            for y_part in range(y_parts):
                first = (channel * y_parts + y_part) * z_parts
                pieces = [blocks_ref[first + i, c * SUBLANES : (c + 1) * SUBLANES, :] for i in range(z_parts)]
                rows += swap_groups(pieces, width)
            parts.append(jnp.concatenate(rows, axis=0))
        zero = jnp.zeros_like(parts[0])
        lone = jnp.where(special, zero, parts[1])
        planes.append((parts[0], lone))
        planes.append((jnp.where(special, parts[1], parts[0]), lone))
        for c in range(2, comps, 2):
            planes.append((parts[c], parts[c + 1]))
    return spectrum(planes, n, zh, zr, yb, 4)


def product_kernel(
    place_ref, blocks_ref, far_ref, near_ref, zh, zr, yb, out_ref, ligand_ref, sems, *, channels, y_parts, z_parts
):
    n = zh.shape[0] // 2
    width = n // z_parts
    groups = LANES // width
    slots = near_ref.shape[1] // (2 * channels * n)
    last = ligand_ref.shape[0]
    special = place_ref[0] == 0
    copies = [pltpu.make_async_copy(far_ref.at[i], ligand_ref.at[i], sems.at[i]) for i in range(last)]
    for copy in copies:
        copy.start()
    receptor = receptor_spectrum(special, blocks_ref, zh, zr, yb, channels, y_parts, z_parts)
    for copy in copies:
        copy.wait()

    for step in range(last + 1):
        ligand = near_ref if step == last else ligand_ref.at[step]
        columns = []
        for rotation in range(2):
            for slot in range(slots):
                real, imag = 0.0, 0.0
                for channel in range(channels):
                    f = receptor[channel * (slots + 1) + (rotation if slot == 0 else slot + 1)]
                    at = ((rotation * channels + channel) * slots + slot) * n
                    fr, fi = f[:n], f[n:]
                    hr, hi = ligand[:n, at : at + n], ligand[n:, at : at + n]
                    real = real + (fr * hr + fi * hi)
                    imag = imag + (fr * hi - fi * hr)
                columns.append(jnp.concatenate([real, imag], axis=0))
        columns = constant_times(yb, columns)
        rows = jnp.concatenate([jnp.concatenate([c[:n], c[n:]], axis=1) for c in columns], axis=0)
        rows = times_constant(rows, zh, zr)
        maps = []
        for i in range(2 * slots):
            both = rows[i * n : (i + 1) * n]
            maps += [both[:, :n], both[:, n:]]
        lone, other = maps[1], maps[2 * slots]
        maps[1], maps[2 * slots] = jnp.where(special, other, lone), jnp.where(special, lone, other)
        for i, plane in enumerate(maps):
            rotation, component = divmod(i, 2 * slots)
            row = (step * 2 * slots + component) * SUBLANES
            for y_part in range(y_parts):
                first = y_part * groups
                pieces = [plane[(first + g) * SUBLANES : (first + g + 1) * SUBLANES] for g in range(groups)]
                for z_part, block in enumerate(swap_groups(pieces, width)):
                    out_ref[(rotation * y_parts + y_part) * z_parts + z_part, row : row + SUBLANES] = block


def inverse_x_kernel(blocks_ref, matrix_ref, out_ref, best_ref, rows_ref, held_ref, sems):
    rotations, _, z_block, n = held_ref.shape
    groups = LANES // z_block
    count = rows_ref.shape[1] // blocks_ref.shape[0]
    copies = [pltpu.make_async_copy(held_ref.at[i], out_ref.at[i], sems.at[i]) for i in range(rotations)]
    for i, copy in enumerate(copies):
        rows_ref[i] = blocks_ref[:, i * count : (i + 1) * count, :].reshape(rows_ref.shape[1:])
        best = None
        for row in range(SUBLANES):
            values = rows_ref[i, pl.ds(row, n, stride=SUBLANES), :]
            result = dot(jnp.concatenate(split(values.T), axis=1), matrix_ref[...])
            result = result[:, :n] + result[:, n:]
            for g in range(groups):
                held_ref[i, g * SUBLANES + row] = result[g * z_block : (g + 1) * z_block, :]
            best = result if best is None else jnp.maximum(best, result)
        copy.start()
        best_ref[i] = jnp.max(best)
    for copy in copies:
        copy.wait()


def whole():
    return pl.BlockSpec(memory_space=pltpu.VMEM)


def room(mebibytes):
    return pltpu.CompilerParams(vmem_limit_bytes=mebibytes << 20)


def far():
    return pl.BlockSpec(memory_space=pltpu.HBM)


def scalars():
    return pl.BlockSpec(memory_space=pltpu.SMEM)


def component_tables(n, comps):
    matrix = forward_x_matrix(n).reshape(n // comps, comps, n)
    head, rest = split_constant(matrix)
    last = (matrix - head.astype(np.float64) - rest.astype(np.float64)).astype(jnp.bfloat16)
    return np.concatenate([head, rest, last, np.zeros_like(head)], axis=1)


def on_device(receptor_grids, ligand_cells, atom_shape, atom_charges, *, sizes):
    n = receptor_grids.shape[1]
    rots, y_parts, z_parts = (sizes[a] for a in AXES)
    devices = rots * y_parts * z_parts
    slots = n // 2 // devices
    comps = 2 * slots
    rows = comps * SUBLANES
    y_block, z_block = receptor_grids.shape[2:]
    rotations, atoms = ligand_cells.shape
    channels = 2
    f32 = jnp.float32
    matrices = split_constant(plus_matrix(n))
    matrices = [jnp.asarray(m) for m in (*matrices, np.concatenate([m.T for m in matrices], axis=0))]
    place = lax.axis_index(AXES).reshape(1)

    components = pl.pallas_call(
        forward_x_kernel,
        out_shape=jax.ShapeDtypeStruct((n * SUBLANES, LANES), f32),
        in_specs=[whole()] * 3,
        out_specs=whole(),
        compiler_params=room(60),
        name="forward_x",
    )(jnp.transpose(receptor_grids, (0, 2, 3, 1)), *(jnp.asarray(m) for m in split_constant(forward_x_matrix(n))))
    components, cells = lax.optimization_barrier((components, ligand_cells))
    other = lax.ppermute(cells, "rot", [(i, i ^ 1) for i in range(rots)])
    blocks = lax.all_to_all(components.reshape(devices, rows, LANES), AXES, 0, 0, tiled=True)

    width = 2 * slots * channels * n
    slabs = max(rotations, VMEM_BYTES // (2 * n * width * 4))
    far_ligand, near_ligand = pl.pallas_call(
        ligand_kernel,
        grid=(rotations,),
        out_shape=[
            jax.ShapeDtypeStruct((slabs, 2 * n, width), f32),
            jax.ShapeDtypeStruct((2 * n, width), f32),
        ],
        in_specs=[scalars()] + [whole()] * 8,
        out_specs=[far(), whole()],
        scratch_shapes=[pltpu.VMEM((rotations - 1, 2 * n, width), f32), pltpu.SemaphoreType.DMA((rotations - 1,))],
        compiler_params=room(24),
        name="ligand",
    )(
        place,
        ligand_cells,
        other,
        atom_shape.reshape(1, atoms),
        atom_charges.reshape(1, atoms),
        jnp.asarray(component_tables(n, comps)),
        *matrices,
    )

    sent = pl.pallas_call(
        functools.partial(product_kernel, channels=channels, y_parts=y_parts, z_parts=z_parts),
        out_shape=jax.ShapeDtypeStruct((devices, rotations * rows, LANES), f32),
        in_specs=[scalars(), whole(), far()] + [whole()] * 4,
        out_specs=whole(),
        scratch_shapes=[pltpu.VMEM((rotations - 1, 2 * n, width), f32), pltpu.SemaphoreType.DMA((rotations - 1,))],
        compiler_params=room(16),
        name="product",
    )(place, blocks, far_ligand, near_ligand, *matrices)
    head, rest = split_constant(inverse_x_matrix(n))
    got = lax.all_to_all(sent, AXES, 0, 0, tiled=True)

    correlation, best = pl.pallas_call(
        inverse_x_kernel,
        out_shape=[
            jax.ShapeDtypeStruct((rotations, y_block, z_block, n), f32),
            jax.ShapeDtypeStruct((rotations,), f32),
        ],
        in_specs=[whole()] * 2,
        out_specs=[far(), scalars()],
        scratch_shapes=[
            pltpu.VMEM((rotations, devices * rows, LANES), f32),
            pltpu.VMEM((rotations, y_block, z_block, n), f32),
            pltpu.SemaphoreType.DMA((rotations,)),
        ],
        compiler_params=room(12),
        name="inverse_x",
    )(got, jnp.asarray(np.block([[head, rest], [head, np.zeros_like(head)]])))
    for axis in ("py", "pz"):
        step = 1
        while step < sizes[axis]:
            best = jnp.maximum(best, lax.ppermute(best, axis, [(i, i ^ step) for i in range(sizes[axis])]))
            step *= 2
    return correlation, best


def twiddle(length, inverse):
    counter = jnp.arange(length, dtype=jnp.int32)
    phases = counter[:, None] * counter[None, :] % length
    angles = phases.astype(jnp.float32) * (2.0 * math.pi / length)
    factor = 1.0 if inverse else -1.0
    return (jnp.cos(angles), factor * jnp.sin(angles))


def transform(real_part, imag_part, pattern, inverse, n):
    cosine, sine_table = twiddle(n, inverse)
    if imag_part is None:
        return (
            jnp.einsum(pattern, real_part, cosine, precision=exact_mode),
            jnp.einsum(pattern, real_part, sine_table, precision=exact_mode),
        )
    new_real = jnp.einsum(pattern, real_part, cosine, precision=exact_mode) - jnp.einsum(
        pattern, imag_part, sine_table, precision=exact_mode
    )
    new_imag = jnp.einsum(pattern, real_part, sine_table, precision=exact_mode) + jnp.einsum(
        pattern, imag_part, cosine, precision=exact_mode
    )
    return (new_real, new_imag)


def exchange(pair, axis, split_axis, concat_axis):
    return tuple(lax.all_to_all(p, axis, split_axis=split_axis, concat_axis=concat_axis, tiled=True) for p in pair)


def on_any_device(receptor_grids, ligand_cells, atom_shape, atom_charges, *, sizes):
    n = receptor_grids.shape[1]
    planes = lax.all_gather(receptor_grids, "rot", axis=0, tiled=True)
    pair = transform(planes, None, "cxyz,xk->ckyz", False, n)
    pair = transform(*exchange(pair, "pz", 1, 3), "cxyz,zk->cxyk", False, n)
    receptor_real, receptor_imag = transform(*exchange(pair, "py", 3, 2), "cxyz,yk->cxkz", False, n)
    x_block = n // sizes["pz"]
    z_block = n // sizes["py"]
    kx_values = lax.axis_index("pz") * x_block + jnp.arange(x_block, dtype=jnp.int32)
    kz_values = lax.axis_index("py") * z_block + jnp.arange(z_block, dtype=jnp.int32)
    ky_values = jnp.arange(n, dtype=jnp.int32)
    weights = jnp.stack((atom_shape, atom_charges), 1)
    step_angle = 2.0 * math.pi / n

    def rotation_product(atom_cells):
        coord_x = atom_cells // (n * n)
        coord_y = atom_cells // n % n
        coord_z = atom_cells % n
        angle_y = (coord_y[:, None] * ky_values[None, :] % n).astype(jnp.float32) * step_angle
        cos_y = jnp.cos(angle_y)
        sin_y = jnp.sin(angle_y)
        phase_xz = (
            coord_x[:, None, None] * kx_values[None, :, None]
            + coord_z[:, None, None] * kz_values[None, None, :]
        ) % n
        angle_xz = phase_xz.astype(jnp.float32) * step_angle
        cos_xz = (weights[:, :, None, None] * jnp.cos(angle_xz)[:, None]).reshape(atom_cells.shape[0], -1)
        sin_xz = (weights[:, :, None, None] * jnp.sin(angle_xz)[:, None]).reshape(atom_cells.shape[0], -1)
        meet = functools.partial(jnp.einsum, "ay,ab->yb", precision=exact_mode)
        conj_real = (meet(cos_y, cos_xz) - meet(sin_y, sin_xz)).reshape(n, 2, x_block, z_block)
        conj_imag = (meet(cos_y, sin_xz) + meet(sin_y, cos_xz)).reshape(n, 2, x_block, z_block)
        join = functools.partial(jnp.einsum, "ycxz,cxyz->xyz", precision=exact_mode)
        product_real = join(conj_real, receptor_real) - join(conj_imag, receptor_imag)
        product_imag = join(conj_imag, receptor_real) + join(conj_real, receptor_imag)
        return (product_real, product_imag)

    product_real, product_imag = lax.map(rotation_product, ligand_cells)
    rotations = ligand_cells.shape[0]
    pair_real = product_real.reshape((rotations // 2, 2) + product_real.shape[1:])
    pair_imag = product_imag.reshape((rotations // 2, 2) + product_imag.shape[1:])
    pair = (pair_real[:, 0] - pair_imag[:, 1], pair_imag[:, 0] + pair_real[:, 1])
    pair = transform(*pair, "bxyz,yk->bxkz", True, n)
    pair = transform(*exchange(pair, "py", 2, 3), "bxyz,zk->bxyk", True, n)
    even_maps, odd_maps = transform(*exchange(pair, "pz", 3, 1), "bxyz,xk->byzk", True, n)
    stacked = jnp.stack((even_maps, odd_maps), 1)
    correlation = stacked.reshape((rotations,) + even_maps.shape[1:]) * (1.0 / (n * n * n))
    best_score = lax.pmax(jnp.max(correlation, axis=(1, 2, 3)), ("py", "pz"))
    return (correlation, best_score)


def solution(mesh):
    sizes = dict(mesh.shape)
    placed = (P("rot", None, "py", "pz"), P("rot", None), P(), P())

    def run(receptor_grids, ligand_cells, atom_shape, atom_charges):
        n = receptor_grids.shape[1]
        devices = math.prod(sizes[a] for a in AXES)
        fits = (
            sizes["rot"] == 2
            and n == LANES
            and (n // 2) % devices == 0
            and (n // sizes["py"]) * (n // sizes["pz"]) == SUBLANES * LANES
            and all(sizes[a] & (sizes[a] - 1) == 0 for a in AXES)
        )
        step = jax.shard_map(
            functools.partial(on_device if fits else on_any_device, sizes=sizes),
            mesh=mesh,
            in_specs=placed,
            out_specs=(P("rot", "py", "pz", None), P("rot")),
            check_vma=False,
        )
        return step(receptor_grids, ligand_cells, atom_shape, atom_charges)

    return run
```

```python
import functools
import math

import jax
import jax.numpy as jnp
import numpy as np
from jax import lax
from jax.experimental import pallas as pl
from jax.experimental.pallas import tpu as pltpu
from jax.sharding import PartitionSpec as P

exact_mode = lax.Precision.HIGHEST
AXES = ("rot", "py", "pz")
LANES = 128
SUBLANES = 8
VMEM_BYTES = 48 << 20


def split_constant(matrix):
    head = np.asarray(matrix, np.float64).astype(jnp.bfloat16)
    rest = (np.asarray(matrix, np.float64) - head.astype(np.float64)).astype(jnp.bfloat16)
    return head, rest


def plus_matrix(n):
    turns = np.outer(np.arange(n), np.arange(n)) % n
    cosine, sine = np.cos(turns * (2 * np.pi / n)), np.sin(turns * (2 * np.pi / n))
    return np.block([[cosine, sine], [-sine, cosine]])


def component_phases(n):
    places = np.arange(n)
    phases = np.zeros((n, n), np.int64)
    for slot in range(n // 2):
        phases[2 * slot] = slot * places % n
        phases[2 * slot + 1] = (n // 2) * places % n if slot == 0 else (slot * places - n // 4) % n
    return phases


def forward_x_matrix(n):
    return np.cos(component_phases(n) * (2 * np.pi / n))


def inverse_x_matrix(n):
    matrix = np.cos(component_phases(n) * (2 * np.pi / n))
    scale = np.full((n, 1), 2.0)
    scale[3::2] = -2.0
    scale[:2] = 1.0
    return matrix * scale / float(n) ** 3


def split(value):
    head = value.astype(jnp.bfloat16)
    rest = (value - head.astype(jnp.float32)).astype(jnp.bfloat16)
    return head, rest


def dot(a, b):
    return jnp.dot(a, b, preferred_element_type=jnp.float32)


def dot_rows(a, b):
    return lax.dot_general(a, b, (((1,), (1,)), ((), ())), preferred_element_type=jnp.float32)


def times_constant(value, head_ref, rest_ref):
    head, rest = split(value)
    count = value.shape[0]
    both = dot(jnp.concatenate([head, rest], axis=0), head_ref[...])
    return both[:count] + (dot(head, rest_ref[...]) + both[count:])


def constant_times(both_ref, values):
    count = both_ref.shape[0] // 2
    results = []
    for i in range(0, len(values), 2):
        pair = values[i : i + 2]
        head, rest = split(jnp.concatenate(pair, axis=1))
        both = dot(both_ref[...], head)
        result = both[:count] + (both[count:] + dot(both_ref[:count], rest))
        width = pair[0].shape[1]
        results += [result[:, j * width : (j + 1) * width] for j in range(len(pair))]
    return results


def swap_groups(pieces, width):
    pieces = list(pieces)
    lane = lax.broadcasted_iota(jnp.int32, pieces[0].shape, 1)
    bit = len(pieces) // 2
    while bit:
        low = lane // (bit * width) % 2 == 0
        for i in range(len(pieces)):
            if i & bit == 0:
                first, second = pieces[i], pieces[i | bit]
                pieces[i] = jnp.where(low, first, pltpu.roll(second, bit * width, 1))
                pieces[i | bit] = jnp.where(low, pltpu.roll(first, LANES - bit * width, 1), second)
        bit //= 2
    return pieces


def forward_x_kernel(grid_ref, head_ref, rest_ref, out_ref):
    y_block, z_block, n = grid_ref.shape[1:]
    groups = LANES // z_block
    high = y_block // groups
    for row in range(high):
        values = jnp.concatenate([grid_ref[0, g * high + row] for g in range(groups)], axis=0)
        head, rest = split(values)
        out_ref[pl.ds(row, n, stride=high), :] = dot_rows(head_ref[...], head) + (
            dot_rows(rest_ref[...], head) + dot_rows(head_ref[...], rest)
        )


def one_hot_rows(count, place):
    rows = lax.broadcasted_iota(jnp.int32, (count, place.shape[1]), 0)
    return jnp.where(rows == place, 1.0, 0.0).astype(jnp.bfloat16)


def spectrum(planes, n, zh, zr, yb, at_once):
    columns = []
    for i in range(0, len(planes), at_once):
        pairs = planes[i : i + at_once]
        rows = jnp.concatenate([jnp.concatenate(pair, axis=1) for pair in pairs], axis=0)
        rows = times_constant(rows, zh, zr)
        columns += [
            jnp.concatenate([rows[j * n : (j + 1) * n, :n], rows[j * n : (j + 1) * n, n:]], axis=0)
            for j in range(len(pairs))
        ]
    return constant_times(yb, columns)


def cosine(turns, n):
    folded = (jnp.abs((turns + n // 2) % n - n // 2) - n // 4).astype(jnp.float32) * (2.0 * math.pi / n)
    square = folded * folded
    total = jnp.zeros_like(folded)
    for power in (13, 11, 9, 7, 5, 3, 1):
        total = total * square + (-1.0) ** ((power + 1) // 2) / math.factorial(power)
    return total * folded


def ligand_kernel(place_ref, cells_ref, shape_ref, charge_ref, zh, zr, yb, far_ref, near_ref, held_ref, sems):
    n = zh.shape[0] // 2
    half = n // 2
    atoms = cells_ref.shape[1]
    comps = near_ref.shape[1] // (2 * n)
    step = pl.program_id(0)
    row = lax.broadcasted_iota(jnp.int32, (comps, 1), 0)
    slot = place_ref[0] * (comps // 2) + row // 2
    second = row % 2 == 1
    times = jnp.where(second & (slot == 0), half, slot)
    shift = jnp.where(second & (slot != 0), n - n // 4, 0)
    special = place_ref[0] == 0
    grids = []
    for rotation in range(2):
        cell = cells_ref[pl.ds(2 * step + rotation, 1), :]
        coord_x, coord_y, coord_z = cell // (n * n), cell // n % n, cell % n
        wave = cosine(times * coord_x + shift, n)
        values = jnp.concatenate([wave * shape_ref[...], wave * charge_ref[...]], axis=0)
        count = values.shape[0]
        head = values.astype(jnp.bfloat16).astype(jnp.float32)
        hit = lax.broadcasted_iota(jnp.int32, (half, atoms), 0) == coord_y % half
        stacked = jnp.concatenate(
            [
                jnp.where(hit, part[c : c + 1, :], 0.0).astype(jnp.bfloat16)
                for part in (head, values - head)
                for c in range(count)
            ],
            axis=0,
        )
        total = dot_rows(stacked, one_hot_rows(2 * n, coord_z + n * (coord_y // half)))
        total = total[: count * half] + total[count * half :]
        grids.append(
            [
                jnp.concatenate(
                    [total[c * half : (c + 1) * half, :n], total[c * half : (c + 1) * half, n:]], axis=0
                )
                for c in range(count)
            ]
        )
    planes = [[], []]
    for c in range(0, count, 2):
        first, second = (grids[0][c], grids[0][c + 1]), (grids[1][c], grids[1][c + 1])
        if c % comps == 0:
            first, second = (
                (first[0], jnp.where(special, second[0], first[1])),
                (jnp.where(special, first[1], second[0]), second[1]),
            )
        planes[0].append(first)
        planes[1].append(second)
    near_ref[...] = jnp.concatenate(spectrum(planes[0] + planes[1], n, zh, zr, yb, 2), axis=1)
    last = pl.num_programs(0) - 1

    @pl.when(step < last)
    def _():
        held_ref[step] = near_ref[...]
        pltpu.make_async_copy(held_ref.at[step], far_ref.at[step], sems.at[step]).start()

    @pl.when(step == last)
    def _():
        for i in range(held_ref.shape[0]):
            pltpu.make_async_copy(held_ref.at[i], far_ref.at[i], sems.at[i]).wait()


def receptor_spectrum(special, blocks_ref, zh, zr, yb, channels, y_parts, z_parts):
    n = zh.shape[0] // 2
    width = n // z_parts
    comps = blocks_ref.shape[1] // SUBLANES
    planes = []
    for channel in range(channels):
        parts = []
        for c in range(comps):
            rows = []
            for y_part in range(y_parts):
                first = (channel * y_parts + y_part) * z_parts
                pieces = [blocks_ref[first + i, c * SUBLANES : (c + 1) * SUBLANES, :] for i in range(z_parts)]
                rows += swap_groups(pieces, width)
            parts.append(jnp.concatenate(rows, axis=0))
        zero = jnp.zeros_like(parts[0])
        lone = jnp.where(special, zero, parts[1])
        planes.append((parts[0], lone))
        planes.append((jnp.where(special, parts[1], parts[0]), lone))
        for c in range(2, comps, 2):
            planes.append((parts[c], parts[c + 1]))
    return spectrum(planes, n, zh, zr, yb, 4)


def product_kernel(
    place_ref,
    blocks_ref,
    far_own_ref,
    near_own_ref,
    far_other_ref,
    near_other_ref,
    zh,
    zr,
    yb,
    out_ref,
    ligand_ref,
    sems,
    *,
    channels,
    y_parts,
    z_parts,
):
    n = zh.shape[0] // 2
    width = n // z_parts
    groups = LANES // width
    slots = near_own_ref.shape[1] // (2 * channels * n)
    pairs = ligand_ref.shape[1] + 1
    special = place_ref[0] == 0
    copies = [
        pltpu.make_async_copy(far.at[i], ligand_ref.at[k, i], sems.at[k, i])
        for k, far in enumerate((far_own_ref, far_other_ref))
        for i in range(pairs - 1)
    ]
    for copy in copies:
        copy.start()
    receptor = receptor_spectrum(special, blocks_ref, zh, zr, yb, channels, y_parts, z_parts)
    for copy in copies:
        copy.wait()
    own = place_ref[0] // (y_parts * z_parts)

    for step in range(2 * pairs):
        k, pair = divmod(step, pairs)
        near_ref = (near_own_ref, near_other_ref)[k]
        ligand = near_ref if pair == pairs - 1 else ligand_ref.at[k, pair]
        device = (1 - own if k else own) * y_parts * z_parts
        for slot in range(slots):
            columns = []
            for rotation in range(2):
                real, imag = 0.0, 0.0
                for channel in range(channels):
                    f = receptor[channel * (slots + 1) + (rotation if slot == 0 else slot + 1)]
                    at = ((rotation * channels + channel) * slots + slot) * n
                    fr, fi = f[:n], f[n:]
                    hr, hi = ligand[:n, at : at + n], ligand[n:, at : at + n]
                    real = real + (fr * hr + fi * hi)
                    imag = imag + (fr * hi - fi * hr)
                columns.append(jnp.concatenate([real, imag], axis=0))
            columns = constant_times(yb, columns)
            rows = jnp.concatenate([jnp.concatenate([c[:n], c[n:]], axis=1) for c in columns], axis=0)
            rows = times_constant(rows, zh, zr)
            maps = [rows[:n, :n], rows[:n, n:], rows[n:, :n], rows[n:, n:]]
            if slot == 0:
                maps[1], maps[2] = jnp.where(special, maps[2], maps[1]), jnp.where(special, maps[1], maps[2])
            for i, plane in enumerate(maps):
                rotation, part = divmod(i, 2)
                row = (((2 * pair + rotation) * slots + slot) * 2 + part) * SUBLANES
                for y_part in range(y_parts):
                    first = y_part * groups
                    pieces = [plane[(first + g) * SUBLANES : (first + g + 1) * SUBLANES] for g in range(groups)]
                    for z_part, block in enumerate(swap_groups(pieces, width)):
                        out_ref[device + y_part * z_parts + z_part, row : row + SUBLANES] = block


def inverse_x_kernel(blocks_ref, matrix_ref, out_ref, best_ref, rows_ref, held_ref, sems):
    rotations, _, z_block, n = held_ref.shape
    groups = LANES // z_block
    count = rows_ref.shape[1] // blocks_ref.shape[0]
    copies = [pltpu.make_async_copy(held_ref.at[i], out_ref.at[i], sems.at[i]) for i in range(rotations)]
    for i, copy in enumerate(copies):
        rows_ref[i] = blocks_ref[:, i * count : (i + 1) * count, :].reshape(rows_ref.shape[1:])
        best = None
        for row in range(SUBLANES):
            values = rows_ref[i, pl.ds(row, n, stride=SUBLANES), :]
            result = dot(jnp.concatenate(split(values.T), axis=1), matrix_ref[...])
            result = result[:, :n] + result[:, n:]
            for g in range(groups):
                held_ref[i, g * SUBLANES + row] = result[g * z_block : (g + 1) * z_block, :]
            best = result if best is None else jnp.maximum(best, result)
        copy.start()
        best_ref[i] = jnp.max(best)
    for copy in copies:
        copy.wait()


def whole():
    return pl.BlockSpec(memory_space=pltpu.VMEM)


def room(mebibytes):
    return pltpu.CompilerParams(vmem_limit_bytes=mebibytes << 20)


def far():
    return pl.BlockSpec(memory_space=pltpu.HBM)


def scalars():
    return pl.BlockSpec(memory_space=pltpu.SMEM)


def on_device(receptor_grids, ligand_cells, atom_shape, atom_charges, *, sizes):
    n = receptor_grids.shape[1]
    rots, y_parts, z_parts = (sizes[a] for a in AXES)
    devices = rots * y_parts * z_parts
    slots = n // 2 // devices
    comps = 2 * slots
    rows = comps * SUBLANES
    y_block, z_block = receptor_grids.shape[2:]
    rotations, atoms = ligand_cells.shape
    channels = 2
    f32 = jnp.float32
    matrices = split_constant(plus_matrix(n))
    matrices = [jnp.asarray(m) for m in (*matrices, np.concatenate([m.T for m in matrices], axis=0))]
    place = lax.axis_index(AXES).reshape(1)

    components = pl.pallas_call(
        forward_x_kernel,
        out_shape=jax.ShapeDtypeStruct((n * SUBLANES, LANES), f32),
        in_specs=[whole()] * 3,
        out_specs=whole(),
        compiler_params=room(60),
        name="forward_x",
    )(jnp.transpose(receptor_grids, (0, 2, 3, 1)), *(jnp.asarray(m) for m in split_constant(forward_x_matrix(n))))
    components, cells = lax.optimization_barrier((components, ligand_cells))
    other = lax.ppermute(cells, "rot", [(i, i ^ 1) for i in range(rots)])
    blocks = lax.all_to_all(components.reshape(devices, rows, LANES), AXES, 0, 0, tiled=True)

    width = 2 * slots * channels * n
    pairs = rotations // 2
    slabs = max(pairs, VMEM_BYTES // (2 * n * width * 4))
    ligand = pl.pallas_call(
        ligand_kernel,
        grid=(pairs,),
        out_shape=[
            jax.ShapeDtypeStruct((slabs, 2 * n, width), f32),
            jax.ShapeDtypeStruct((2 * n, width), f32),
        ],
        in_specs=[scalars()] + [whole()] * 6,
        out_specs=[far(), whole()],
        scratch_shapes=[pltpu.VMEM((pairs - 1, 2 * n, width), f32), pltpu.SemaphoreType.DMA((pairs - 1,))],
        compiler_params=room(24),
        name="ligand",
    )
    weights = (atom_shape.reshape(1, atoms), atom_charges.reshape(1, atoms))
    spectra = (*ligand(place, ligand_cells, *weights, *matrices), *ligand(place, other, *weights, *matrices))

    sent = pl.pallas_call(
        functools.partial(product_kernel, channels=channels, y_parts=y_parts, z_parts=z_parts),
        out_shape=jax.ShapeDtypeStruct((devices, rotations * rows, LANES), f32),
        in_specs=[scalars(), whole(), far(), whole(), far()] + [whole()] * 4,
        out_specs=whole(),
        scratch_shapes=[pltpu.VMEM((2, pairs - 1, 2 * n, width), f32), pltpu.SemaphoreType.DMA((2, pairs - 1))],
        compiler_params=room(16),
        name="product",
    )(place, blocks, *spectra, *matrices)
    head, rest = split_constant(inverse_x_matrix(n))
    got = lax.all_to_all(sent, AXES, 0, 0, tiled=True)

    correlation, best = pl.pallas_call(
        inverse_x_kernel,
        out_shape=[
            jax.ShapeDtypeStruct((rotations, y_block, z_block, n), f32),
            jax.ShapeDtypeStruct((rotations,), f32),
        ],
        in_specs=[whole()] * 2,
        out_specs=[far(), scalars()],
        scratch_shapes=[
            pltpu.VMEM((rotations, devices * rows, LANES), f32),
            pltpu.VMEM((rotations, y_block, z_block, n), f32),
            pltpu.SemaphoreType.DMA((rotations,)),
        ],
        compiler_params=room(12),
        name="inverse_x",
    )(got, jnp.asarray(np.block([[head, rest], [head, np.zeros_like(head)]])))
    for axis in ("py", "pz"):
        step = 1
        while step < sizes[axis]:
            best = jnp.maximum(best, lax.ppermute(best, axis, [(i, i ^ step) for i in range(sizes[axis])]))
            step *= 2
    return correlation, best


def twiddle(length, inverse):
    counter = jnp.arange(length, dtype=jnp.int32)
    phases = counter[:, None] * counter[None, :] % length
    angles = phases.astype(jnp.float32) * (2.0 * math.pi / length)
    factor = 1.0 if inverse else -1.0
    return (jnp.cos(angles), factor * jnp.sin(angles))


def transform(real_part, imag_part, pattern, inverse, n):
    cosine, sine_table = twiddle(n, inverse)
    if imag_part is None:
        return (
            jnp.einsum(pattern, real_part, cosine, precision=exact_mode),
            jnp.einsum(pattern, real_part, sine_table, precision=exact_mode),
        )
    new_real = jnp.einsum(pattern, real_part, cosine, precision=exact_mode) - jnp.einsum(
        pattern, imag_part, sine_table, precision=exact_mode
    )
    new_imag = jnp.einsum(pattern, real_part, sine_table, precision=exact_mode) + jnp.einsum(
        pattern, imag_part, cosine, precision=exact_mode
    )
    return (new_real, new_imag)


def exchange(pair, axis, split_axis, concat_axis):
    return tuple(lax.all_to_all(p, axis, split_axis=split_axis, concat_axis=concat_axis, tiled=True) for p in pair)


def on_any_device(receptor_grids, ligand_cells, atom_shape, atom_charges, *, sizes):
    n = receptor_grids.shape[1]
    planes = lax.all_gather(receptor_grids, "rot", axis=0, tiled=True)
    pair = transform(planes, None, "cxyz,xk->ckyz", False, n)
    pair = transform(*exchange(pair, "pz", 1, 3), "cxyz,zk->cxyk", False, n)
    receptor_real, receptor_imag = transform(*exchange(pair, "py", 3, 2), "cxyz,yk->cxkz", False, n)
    x_block = n // sizes["pz"]
    z_block = n // sizes["py"]
    kx_values = lax.axis_index("pz") * x_block + jnp.arange(x_block, dtype=jnp.int32)
    kz_values = lax.axis_index("py") * z_block + jnp.arange(z_block, dtype=jnp.int32)
    ky_values = jnp.arange(n, dtype=jnp.int32)
    weights = jnp.stack((atom_shape, atom_charges), 1)
    step_angle = 2.0 * math.pi / n

    def rotation_product(atom_cells):
        coord_x = atom_cells // (n * n)
        coord_y = atom_cells // n % n
        coord_z = atom_cells % n
        angle_y = (coord_y[:, None] * ky_values[None, :] % n).astype(jnp.float32) * step_angle
        cos_y = jnp.cos(angle_y)
        sin_y = jnp.sin(angle_y)
        phase_xz = (
            coord_x[:, None, None] * kx_values[None, :, None]
            + coord_z[:, None, None] * kz_values[None, None, :]
        ) % n
        angle_xz = phase_xz.astype(jnp.float32) * step_angle
        cos_xz = (weights[:, :, None, None] * jnp.cos(angle_xz)[:, None]).reshape(atom_cells.shape[0], -1)
        sin_xz = (weights[:, :, None, None] * jnp.sin(angle_xz)[:, None]).reshape(atom_cells.shape[0], -1)
        meet = functools.partial(jnp.einsum, "ay,ab->yb", precision=exact_mode)
        conj_real = (meet(cos_y, cos_xz) - meet(sin_y, sin_xz)).reshape(n, 2, x_block, z_block)
        conj_imag = (meet(cos_y, sin_xz) + meet(sin_y, cos_xz)).reshape(n, 2, x_block, z_block)
        join = functools.partial(jnp.einsum, "ycxz,cxyz->xyz", precision=exact_mode)
        product_real = join(conj_real, receptor_real) - join(conj_imag, receptor_imag)
        product_imag = join(conj_imag, receptor_real) + join(conj_real, receptor_imag)
        return (product_real, product_imag)

    product_real, product_imag = lax.map(rotation_product, ligand_cells)
    rotations = ligand_cells.shape[0]
    pair_real = product_real.reshape((rotations // 2, 2) + product_real.shape[1:])
    pair_imag = product_imag.reshape((rotations // 2, 2) + product_imag.shape[1:])
    pair = (pair_real[:, 0] - pair_imag[:, 1], pair_imag[:, 0] + pair_real[:, 1])
    pair = transform(*pair, "bxyz,yk->bxkz", True, n)
    pair = transform(*exchange(pair, "py", 2, 3), "bxyz,zk->bxyk", True, n)
    even_maps, odd_maps = transform(*exchange(pair, "pz", 3, 1), "bxyz,xk->byzk", True, n)
    stacked = jnp.stack((even_maps, odd_maps), 1)
    correlation = stacked.reshape((rotations,) + even_maps.shape[1:]) * (1.0 / (n * n * n))
    best_score = lax.pmax(jnp.max(correlation, axis=(1, 2, 3)), ("py", "pz"))
    return (correlation, best_score)


def solution(mesh):
    sizes = dict(mesh.shape)
    placed = (P("rot", None, "py", "pz"), P("rot", None), P(), P())

    def run(receptor_grids, ligand_cells, atom_shape, atom_charges):
        n = receptor_grids.shape[1]
        devices = math.prod(sizes[a] for a in AXES)
        fits = (
            sizes["rot"] == 2
            and n == LANES
            and ligand_cells.shape[0] % 4 == 0
            and (n // 2) % devices == 0
            and (n // sizes["py"]) * (n // sizes["pz"]) == SUBLANES * LANES
            and all(sizes[a] & (sizes[a] - 1) == 0 for a in AXES)
        )
        step = jax.shard_map(
            functools.partial(on_device if fits else on_any_device, sizes=sizes),
            mesh=mesh,
            in_specs=placed,
            out_specs=(P("rot", "py", "pz", None), P("rot")),
            check_vma=False,
        )
        return step(receptor_grids, ligand_cells, atom_shape, atom_charges)

    return run
```

```python
import functools
import math

import jax
import jax.numpy as jnp
import numpy as np
from jax import lax
from jax.experimental import pallas as pl
from jax.experimental.pallas import tpu as pltpu
from jax.sharding import PartitionSpec as P

exact_mode = lax.Precision.HIGHEST
AXES = ("rot", "py", "pz")
LANES = 128
SUBLANES = 8
VMEM_BYTES = 48 << 20


def split_constant(matrix):
    head = np.asarray(matrix, np.float64).astype(jnp.bfloat16)
    rest = (np.asarray(matrix, np.float64) - head.astype(np.float64)).astype(jnp.bfloat16)
    return head, rest


def plus_matrix(n):
    turns = np.outer(np.arange(n), np.arange(n)) % n
    cosine, sine = np.cos(turns * (2 * np.pi / n)), np.sin(turns * (2 * np.pi / n))
    return np.block([[cosine, sine], [-sine, cosine]])


def component_phases(n):
    places = np.arange(n)
    phases = np.zeros((n, n), np.int64)
    for slot in range(n // 2):
        phases[2 * slot] = slot * places % n
        phases[2 * slot + 1] = (n // 2) * places % n if slot == 0 else (slot * places - n // 4) % n
    return phases


def forward_x_matrix(n):
    return np.cos(component_phases(n) * (2 * np.pi / n))


def inverse_x_matrix(n):
    matrix = np.cos(component_phases(n) * (2 * np.pi / n))
    scale = np.full((n, 1), 2.0)
    scale[3::2] = -2.0
    scale[:2] = 1.0
    return matrix * scale / float(n) ** 3


def split(value):
    head = value.astype(jnp.bfloat16)
    rest = (value - head.astype(jnp.float32)).astype(jnp.bfloat16)
    return head, rest


def dot(a, b):
    return jnp.dot(a, b, preferred_element_type=jnp.float32)


def dot_rows(a, b):
    return lax.dot_general(a, b, (((1,), (1,)), ((), ())), preferred_element_type=jnp.float32)


def times_constant(value, head_ref, rest_ref):
    head, rest = split(value)
    count = value.shape[0]
    both = dot(jnp.concatenate([head, rest], axis=0), head_ref[...])
    return both[:count] + (dot(head, rest_ref[...]) + both[count:])


def constant_times(both_ref, values):
    count = both_ref.shape[0] // 2
    results = []
    for i in range(0, len(values), 2):
        pair = values[i : i + 2]
        head, rest = split(jnp.concatenate(pair, axis=1))
        both = dot(both_ref[...], head)
        result = both[:count] + (both[count:] + dot(both_ref[:count], rest))
        width = pair[0].shape[1]
        results += [result[:, j * width : (j + 1) * width] for j in range(len(pair))]
    return results


def swap_groups(pieces, width):
    pieces = list(pieces)
    lane = lax.broadcasted_iota(jnp.int32, pieces[0].shape, 1)
    bit = len(pieces) // 2
    while bit:
        low = lane // (bit * width) % 2 == 0
        for i in range(len(pieces)):
            if i & bit == 0:
                first, second = pieces[i], pieces[i | bit]
                pieces[i] = jnp.where(low, first, pltpu.roll(second, bit * width, 1))
                pieces[i | bit] = jnp.where(low, pltpu.roll(first, LANES - bit * width, 1), second)
        bit //= 2
    return pieces


def forward_x_kernel(grid_ref, both_ref, out_ref):
    y_block, z_block, n = grid_ref.shape[1:]
    groups = LANES // z_block
    high = y_block // groups
    for row in range(high):
        values = jnp.concatenate([grid_ref[0, g * high + row] for g in range(groups)], axis=0)
        head, rest = split(values)
        both = dot_rows(both_ref[...], head)
        out_ref[pl.ds(row, n, stride=high), :] = both[:n] + (both[n:] + dot_rows(both_ref[:n], rest))


def one_hot_rows(count, place):
    rows = lax.broadcasted_iota(jnp.int32, (count, place.shape[1]), 0)
    return jnp.where(rows == place, 1.0, 0.0).astype(jnp.bfloat16)


def spectrum(planes, n, zh, zr, yb, at_once):
    columns = []
    for i in range(0, len(planes), at_once):
        pairs = planes[i : i + at_once]
        rows = jnp.concatenate([jnp.concatenate(pair, axis=1) for pair in pairs], axis=0)
        rows = times_constant(rows, zh, zr)
        columns += [
            jnp.concatenate([rows[j * n : (j + 1) * n, :n], rows[j * n : (j + 1) * n, n:]], axis=0)
            for j in range(len(pairs))
        ]
    return constant_times(yb, columns)


def cosine(turns, n):
    folded = (jnp.abs((turns + n // 2) % n - n // 2) - n // 4).astype(jnp.float32) * (2.0 * math.pi / n)
    square = folded * folded
    total = jnp.zeros_like(folded)
    for power in (13, 11, 9, 7, 5, 3, 1):
        total = total * square + (-1.0) ** ((power + 1) // 2) / math.factorial(power)
    return total * folded


def ligand_kernel(place_ref, cells_ref, shape_ref, charge_ref, zh, zr, yb, far_ref, near_ref, held_ref, sems):
    n = zh.shape[0] // 2
    half = n // 2
    atoms = cells_ref.shape[1]
    comps = near_ref.shape[1] // (2 * n)
    last = held_ref.shape[0]
    copies = [pltpu.make_async_copy(held_ref.at[i], far_ref.at[i], sems.at[i]) for i in range(last)]
    row = lax.broadcasted_iota(jnp.int32, (comps, 1), 0)
    slot = place_ref[0] * (comps // 2) + row // 2
    second = row % 2 == 1
    times = jnp.where(second & (slot == 0), half, slot)
    shift = jnp.where(second & (slot != 0), n - n // 4, 0)
    special = place_ref[0] == 0
    for step in range(last + 1):
        grids = []
        for rotation in range(2):
            cell = cells_ref[2 * step + rotation : 2 * step + rotation + 1, :]
            coord_x, coord_y, coord_z = cell // (n * n), cell // n % n, cell % n
            wave = cosine(times * coord_x + shift, n)
            values = jnp.concatenate([wave * shape_ref[...], wave * charge_ref[...]], axis=0)
            count = values.shape[0]
            head = values.astype(jnp.bfloat16).astype(jnp.float32)
            hit = lax.broadcasted_iota(jnp.int32, (half, atoms), 0) == coord_y % half
            stacked = jnp.concatenate(
                [
                    jnp.where(hit, part[c : c + 1, :], 0.0).astype(jnp.bfloat16)
                    for part in (head, values - head)
                    for c in range(count)
                ],
                axis=0,
            )
            total = dot_rows(stacked, one_hot_rows(2 * n, coord_z + n * (coord_y // half)))
            total = total[: count * half] + total[count * half :]
            grids.append(
                [
                    jnp.concatenate(
                        [total[c * half : (c + 1) * half, :n], total[c * half : (c + 1) * half, n:]], axis=0
                    )
                    for c in range(count)
                ]
            )
        planes = [[], []]
        for c in range(0, count, 2):
            first, second = (grids[0][c], grids[0][c + 1]), (grids[1][c], grids[1][c + 1])
            if c % comps == 0:
                first, second = (
                    (first[0], jnp.where(special, second[0], first[1])),
                    (jnp.where(special, first[1], second[0]), second[1]),
                )
            planes[0].append(first)
            planes[1].append(second)
        spectra = jnp.concatenate(spectrum(planes[0] + planes[1], n, zh, zr, yb, 2), axis=1)
        if step == last:
            near_ref[...] = spectra
        else:
            held_ref[step] = spectra
            copies[step].start()
    for copy in copies:
        copy.wait()


def receptor_spectrum(special, blocks_ref, zh, zr, yb, channels, y_parts, z_parts):
    n = zh.shape[0] // 2
    width = n // z_parts
    comps = blocks_ref.shape[1] // SUBLANES
    planes = []
    for channel in range(channels):
        parts = []
        for c in range(comps):
            rows = []
            for y_part in range(y_parts):
                first = (channel * y_parts + y_part) * z_parts
                pieces = [blocks_ref[first + i, c * SUBLANES : (c + 1) * SUBLANES, :] for i in range(z_parts)]
                rows += swap_groups(pieces, width)
            parts.append(jnp.concatenate(rows, axis=0))
        zero = jnp.zeros_like(parts[0])
        lone = jnp.where(special, zero, parts[1])
        planes.append((parts[0], lone))
        planes.append((jnp.where(special, parts[1], parts[0]), lone))
        for c in range(2, comps, 2):
            planes.append((parts[c], parts[c + 1]))
    return spectrum(planes, n, zh, zr, yb, 4)


def product_kernel(
    place_ref,
    blocks_ref,
    far_own_ref,
    near_own_ref,
    far_other_ref,
    near_other_ref,
    zh,
    zr,
    yb,
    out_ref,
    ligand_ref,
    sems,
    *,
    channels,
    y_parts,
    z_parts,
):
    n = zh.shape[0] // 2
    width = n // z_parts
    groups = LANES // width
    slots = near_own_ref.shape[1] // (2 * channels * n)
    pairs = ligand_ref.shape[1] + 1
    special = place_ref[0] == 0
    copies = [
        pltpu.make_async_copy(far.at[i], ligand_ref.at[k, i], sems.at[k, i])
        for k, far in enumerate((far_own_ref, far_other_ref))
        for i in range(pairs - 1)
    ]
    for copy in copies:
        copy.start()
    receptor = receptor_spectrum(special, blocks_ref, zh, zr, yb, channels, y_parts, z_parts)
    for copy in copies:
        copy.wait()
    own = place_ref[0] // (y_parts * z_parts)

    for step in range(2 * pairs):
        k, pair = divmod(step, pairs)
        near_ref = (near_own_ref, near_other_ref)[k]
        ligand = near_ref if pair == pairs - 1 else ligand_ref.at[k, pair]
        device = (1 - own if k else own) * y_parts * z_parts
        for slot in range(slots):
            columns = []
            for rotation in range(2):
                real, imag = 0.0, 0.0
                for channel in range(channels):
                    f = receptor[channel * (slots + 1) + (rotation if slot == 0 else slot + 1)]
                    at = ((rotation * channels + channel) * slots + slot) * n
                    fr, fi = f[:n], f[n:]
                    hr, hi = ligand[:n, at : at + n], ligand[n:, at : at + n]
                    real = real + (fr * hr + fi * hi)
                    imag = imag + (fr * hi - fi * hr)
                columns.append(jnp.concatenate([real, imag], axis=0))
            columns = constant_times(yb, columns)
            rows = jnp.concatenate([jnp.concatenate([c[:n], c[n:]], axis=1) for c in columns], axis=0)
            rows = times_constant(rows, zh, zr)
            maps = [rows[:n, :n], rows[:n, n:], rows[n:, :n], rows[n:, n:]]
            if slot == 0:
                maps[1], maps[2] = jnp.where(special, maps[2], maps[1]), jnp.where(special, maps[1], maps[2])
            for i, plane in enumerate(maps):
                rotation, part = divmod(i, 2)
                row = (((2 * pair + rotation) * slots + slot) * 2 + part) * SUBLANES
                for y_part in range(y_parts):
                    first = y_part * groups
                    pieces = [plane[(first + g) * SUBLANES : (first + g + 1) * SUBLANES] for g in range(groups)]
                    for z_part, block in enumerate(swap_groups(pieces, width)):
                        out_ref[device + y_part * z_parts + z_part, row : row + SUBLANES] = block


def inverse_x_kernel(blocks_ref, matrix_ref, out_ref, best_ref, rows_ref, held_ref, sems):
    rotations, _, z_block, n = held_ref.shape
    groups = LANES // z_block
    count = rows_ref.shape[1] // blocks_ref.shape[0]
    copies = [pltpu.make_async_copy(held_ref.at[i], out_ref.at[i], sems.at[i]) for i in range(rotations)]
    for i, copy in enumerate(copies):
        rows_ref[i] = blocks_ref[:, i * count : (i + 1) * count, :].reshape(rows_ref.shape[1:])
        best = None
        for row in range(SUBLANES):
            values = rows_ref[i, pl.ds(row, n, stride=SUBLANES), :]
            result = dot(jnp.concatenate(split(values.T), axis=1), matrix_ref[...])
            result = result[:, :n] + result[:, n:]
            for g in range(groups):
                held_ref[i, g * SUBLANES + row] = result[g * z_block : (g + 1) * z_block, :]
            best = result if best is None else jnp.maximum(best, result)
        copy.start()
        best_ref[i] = jnp.max(best)
    for copy in copies:
        copy.wait()


def whole():
    return pl.BlockSpec(memory_space=pltpu.VMEM)


def room(mebibytes):
    return pltpu.CompilerParams(vmem_limit_bytes=mebibytes << 20)


def far():
    return pl.BlockSpec(memory_space=pltpu.HBM)


def scalars():
    return pl.BlockSpec(memory_space=pltpu.SMEM)


def on_device(receptor_grids, ligand_cells, atom_shape, atom_charges, *, sizes):
    n = receptor_grids.shape[1]
    rots, y_parts, z_parts = (sizes[a] for a in AXES)
    devices = rots * y_parts * z_parts
    slots = n // 2 // devices
    comps = 2 * slots
    rows = comps * SUBLANES
    y_block, z_block = receptor_grids.shape[2:]
    rotations, atoms = ligand_cells.shape
    channels = 2
    f32 = jnp.float32
    matrices = split_constant(plus_matrix(n))
    matrices = [jnp.asarray(m) for m in (*matrices, np.concatenate([m.T for m in matrices], axis=0))]
    place = lax.axis_index(AXES).reshape(1)

    components = pl.pallas_call(
        forward_x_kernel,
        out_shape=jax.ShapeDtypeStruct((n * SUBLANES, LANES), f32),
        in_specs=[whole()] * 2,
        out_specs=whole(),
        compiler_params=room(60),
        name="forward_x",
    )(jnp.transpose(receptor_grids, (0, 2, 3, 1)), jnp.asarray(np.concatenate(split_constant(forward_x_matrix(n)), axis=0)))
    components, cells = lax.optimization_barrier((components, ligand_cells))
    other = lax.ppermute(cells, "rot", [(i, i ^ 1) for i in range(rots)])
    blocks = lax.all_to_all(components.reshape(devices, rows, LANES), AXES, 0, 0, tiled=True)

    width = 2 * slots * channels * n
    pairs = rotations // 2
    slabs = max(pairs, VMEM_BYTES // (2 * n * width * 4))
    ligand = pl.pallas_call(
        ligand_kernel,
        out_shape=[
            jax.ShapeDtypeStruct((slabs, 2 * n, width), f32),
            jax.ShapeDtypeStruct((2 * n, width), f32),
        ],
        in_specs=[scalars()] + [whole()] * 6,
        out_specs=[far(), whole()],
        scratch_shapes=[pltpu.VMEM((pairs - 1, 2 * n, width), f32), pltpu.SemaphoreType.DMA((pairs - 1,))],
        compiler_params=room(24),
        name="ligand",
    )
    weights = (atom_shape.reshape(1, atoms), atom_charges.reshape(1, atoms))
    spectra = (*ligand(place, ligand_cells, *weights, *matrices), *ligand(place, other, *weights, *matrices))

    sent = pl.pallas_call(
        functools.partial(product_kernel, channels=channels, y_parts=y_parts, z_parts=z_parts),
        out_shape=jax.ShapeDtypeStruct((devices, rotations * rows, LANES), f32),
        in_specs=[scalars(), whole(), far(), whole(), far()] + [whole()] * 4,
        out_specs=whole(),
        scratch_shapes=[pltpu.VMEM((2, pairs - 1, 2 * n, width), f32), pltpu.SemaphoreType.DMA((2, pairs - 1))],
        compiler_params=room(16),
        name="product",
    )(place, blocks, *spectra, *matrices)
    head, rest = split_constant(inverse_x_matrix(n))
    got = lax.all_to_all(sent, AXES, 0, 0, tiled=True)

    correlation, best = pl.pallas_call(
        inverse_x_kernel,
        out_shape=[
            jax.ShapeDtypeStruct((rotations, y_block, z_block, n), f32),
            jax.ShapeDtypeStruct((rotations,), f32),
        ],
        in_specs=[whole()] * 2,
        out_specs=[far(), scalars()],
        scratch_shapes=[
            pltpu.VMEM((rotations, devices * rows, LANES), f32),
            pltpu.VMEM((rotations, y_block, z_block, n), f32),
            pltpu.SemaphoreType.DMA((rotations,)),
        ],
        compiler_params=room(12),
        name="inverse_x",
    )(got, jnp.asarray(np.block([[head, rest], [head, np.zeros_like(head)]])))
    for axis in ("py", "pz"):
        step = 1
        while step < sizes[axis]:
            best = jnp.maximum(best, lax.ppermute(best, axis, [(i, i ^ step) for i in range(sizes[axis])]))
            step *= 2
    return correlation, best


def twiddle(length, inverse):
    counter = jnp.arange(length, dtype=jnp.int32)
    phases = counter[:, None] * counter[None, :] % length
    angles = phases.astype(jnp.float32) * (2.0 * math.pi / length)
    factor = 1.0 if inverse else -1.0
    return (jnp.cos(angles), factor * jnp.sin(angles))


def transform(real_part, imag_part, pattern, inverse, n):
    cosine, sine_table = twiddle(n, inverse)
    if imag_part is None:
        return (
            jnp.einsum(pattern, real_part, cosine, precision=exact_mode),
            jnp.einsum(pattern, real_part, sine_table, precision=exact_mode),
        )
    new_real = jnp.einsum(pattern, real_part, cosine, precision=exact_mode) - jnp.einsum(
        pattern, imag_part, sine_table, precision=exact_mode
    )
    new_imag = jnp.einsum(pattern, real_part, sine_table, precision=exact_mode) + jnp.einsum(
        pattern, imag_part, cosine, precision=exact_mode
    )
    return (new_real, new_imag)


def exchange(pair, axis, split_axis, concat_axis):
    return tuple(lax.all_to_all(p, axis, split_axis=split_axis, concat_axis=concat_axis, tiled=True) for p in pair)


def on_any_device(receptor_grids, ligand_cells, atom_shape, atom_charges, *, sizes):
    n = receptor_grids.shape[1]
    planes = lax.all_gather(receptor_grids, "rot", axis=0, tiled=True)
    pair = transform(planes, None, "cxyz,xk->ckyz", False, n)
    pair = transform(*exchange(pair, "pz", 1, 3), "cxyz,zk->cxyk", False, n)
    receptor_real, receptor_imag = transform(*exchange(pair, "py", 3, 2), "cxyz,yk->cxkz", False, n)
    x_block = n // sizes["pz"]
    z_block = n // sizes["py"]
    kx_values = lax.axis_index("pz") * x_block + jnp.arange(x_block, dtype=jnp.int32)
    kz_values = lax.axis_index("py") * z_block + jnp.arange(z_block, dtype=jnp.int32)
    ky_values = jnp.arange(n, dtype=jnp.int32)
    weights = jnp.stack((atom_shape, atom_charges), 1)
    step_angle = 2.0 * math.pi / n

    def rotation_product(atom_cells):
        coord_x = atom_cells // (n * n)
        coord_y = atom_cells // n % n
        coord_z = atom_cells % n
        angle_y = (coord_y[:, None] * ky_values[None, :] % n).astype(jnp.float32) * step_angle
        cos_y = jnp.cos(angle_y)
        sin_y = jnp.sin(angle_y)
        phase_xz = (
            coord_x[:, None, None] * kx_values[None, :, None]
            + coord_z[:, None, None] * kz_values[None, None, :]
        ) % n
        angle_xz = phase_xz.astype(jnp.float32) * step_angle
        cos_xz = (weights[:, :, None, None] * jnp.cos(angle_xz)[:, None]).reshape(atom_cells.shape[0], -1)
        sin_xz = (weights[:, :, None, None] * jnp.sin(angle_xz)[:, None]).reshape(atom_cells.shape[0], -1)
        meet = functools.partial(jnp.einsum, "ay,ab->yb", precision=exact_mode)
        conj_real = (meet(cos_y, cos_xz) - meet(sin_y, sin_xz)).reshape(n, 2, x_block, z_block)
        conj_imag = (meet(cos_y, sin_xz) + meet(sin_y, cos_xz)).reshape(n, 2, x_block, z_block)
        join = functools.partial(jnp.einsum, "ycxz,cxyz->xyz", precision=exact_mode)
        product_real = join(conj_real, receptor_real) - join(conj_imag, receptor_imag)
        product_imag = join(conj_imag, receptor_real) + join(conj_real, receptor_imag)
        return (product_real, product_imag)

    product_real, product_imag = lax.map(rotation_product, ligand_cells)
    rotations = ligand_cells.shape[0]
    pair_real = product_real.reshape((rotations // 2, 2) + product_real.shape[1:])
    pair_imag = product_imag.reshape((rotations // 2, 2) + product_imag.shape[1:])
    pair = (pair_real[:, 0] - pair_imag[:, 1], pair_imag[:, 0] + pair_real[:, 1])
    pair = transform(*pair, "bxyz,yk->bxkz", True, n)
    pair = transform(*exchange(pair, "py", 2, 3), "bxyz,zk->bxyk", True, n)
    even_maps, odd_maps = transform(*exchange(pair, "pz", 3, 1), "bxyz,xk->byzk", True, n)
    stacked = jnp.stack((even_maps, odd_maps), 1)
    correlation = stacked.reshape((rotations,) + even_maps.shape[1:]) * (1.0 / (n * n * n))
    best_score = lax.pmax(jnp.max(correlation, axis=(1, 2, 3)), ("py", "pz"))
    return (correlation, best_score)


def solution(mesh):
    sizes = dict(mesh.shape)
    placed = (P("rot", None, "py", "pz"), P("rot", None), P(), P())

    def run(receptor_grids, ligand_cells, atom_shape, atom_charges):
        n = receptor_grids.shape[1]
        devices = math.prod(sizes[a] for a in AXES)
        fits = (
            sizes["rot"] == 2
            and n == LANES
            and ligand_cells.shape[0] % 4 == 0
            and (n // 2) % devices == 0
            and (n // sizes["py"]) * (n // sizes["pz"]) == SUBLANES * LANES
            and all(sizes[a] & (sizes[a] - 1) == 0 for a in AXES)
        )
        step = jax.shard_map(
            functools.partial(on_device if fits else on_any_device, sizes=sizes),
            mesh=mesh,
            in_specs=placed,
            out_specs=(P("rot", "py", "pz", None), P("rot")),
            check_vma=False,
        )
        return step(receptor_grids, ligand_cells, atom_shape, atom_charges)

    return run
```
